256 devices in a mesh: gx: 8 (over x, core), gy: 8 (over z_lo, y), gz: 4 (over z_hi).
Axes of the slice: x: 4, y: 4, z: 8 (z_hi: 4, z_lo: 2; z = z_hi * 2 + z_lo), core: 2. Of those that a mesh axis runs over, the one named last changes fastest.
Arguments:
- grid_inputs: bfloat16 [186, 512, 1024], P(None, 'gx', 'gy'), may hold values from -6 to 6
- embed_w1: bfloat16 [512, 186], replicated, may hold values from -0.4375 to 0.4375
- embed_b1: float32 [512], replicated, may hold values from -3 to 3
- embed_w2: bfloat16 [512, 512], replicated, may hold values from -0.25 to 0.25
- embed_gain: float32 [512], replicated, may hold values from 0.1 to 1.9
- edge_w1: bfloat16 [512, 1536], replicated, may hold values from -0.15625 to 0.15625
- edge_b1: float32 [512], replicated, may hold values from -3 to 3
- edge_w2: bfloat16 [512, 512], replicated, may hold values from -0.25 to 0.25
- message_gain: float32 [512], replicated, may hold values from 0.1 to 1.9
- message_bias: float32 [512], replicated, may hold values from -3 to 3
- mesh_latent: bfloat16 [512, 8, 8, 256], P('gz', 'gx', 'gy'), may hold values from -6 to 6
- edge_latent: bfloat16 [512, 8, 8, 2048], P('gz', 'gx', 'gy'), may hold values from -6 to 6
- senders: int32 [8, 8, 2048], P('gx', 'gy'), may hold values from 0 to 524287, as said below
- receivers: int32 [8, 8, 2048], P('gx', 'gy'), may hold values from 0 to 16383, as said below
- edge_counts: int32 [8, 8], P('gx', 'gy'), may hold values from 1 to 2048, as said below
Outputs:
- mesh_out: bfloat16 [512, 8, 8, 256], P('gz', 'gx', 'gy')
- grid_latent: bfloat16 [512, 512, 1024], P('gz', 'gx', 'gy')
The draws below stay inside these ranges and needn't reach their ends.
Inputs may be any that keep to these rules, and one draw needn't show every extreme that they name: `senders`: an edge of tile (b, c) has its sender's row within 8 rows of rows b * 64 to (b + 1) * 64 - 1, clipped to the grid, and its column within 8 columns, cyclically, of columns c * 128 to (c + 1) * 128 - 1; this holds in every slot. `receivers`: an edge of tile t is received by a node of that tile, t * 256 to (t + 1) * 256 - 1, in every slot. `edge_counts`: the live edges of a tile are its first slots; some tile holds 2048 live edges.
All inputs are finite; a program needn't handle non-finite values.
Results may differ from the reference program's by a relative error of at most 0.0049.
Values may be sent and summed in bfloat16 or wider, within the bound.
A program may use at most 128 MiB of HBM per device.

```python
import jax
import jax.numpy as jnp
from jax import lax

LATENT = 512
CHANNELS = 186
GLAT = 64
GLON = 128
MESH_DEV = 256
EDGE_DEV = 2048
HALO = 8
BANDS = 8
SECTORS = 8
NLAT = 512
NLON = 1024


def tile_coords():
    band_ids = jnp.arange(BANDS, dtype=jnp.int32)[:, None, None]
    sector_ids = jnp.arange(SECTORS, dtype=jnp.int32)[None, :, None]
    return (band_ids, sector_ids)


def draw_senders(key, part):
    band_ids, sector_ids = tile_coords()
    lat_key, lon_key = jax.random.split(jax.random.fold_in(key, 11))
    shape = (BANDS, SECTORS, EDGE_DEV)
    rows = jax.random.randint(lat_key, shape, 0, GLAT + 2 * HALO, dtype=jnp.int32) + band_ids * GLAT - HALO
    rows = jnp.clip(rows, 0, NLAT - 1)
    columns = jax.random.randint(lon_key, shape, 0, GLON + 2 * HALO, dtype=jnp.int32) + sector_ids * GLON - HALO + NLON
    columns = columns % NLON
    return (rows * NLON + columns).astype(jnp.int32)


def draw_receivers(key, part):
    band_ids, sector_ids = tile_coords()
    first_key, second_key = jax.random.split(jax.random.fold_in(key, 23))
    shape = (BANDS, SECTORS, EDGE_DEV)
    first = jax.random.randint(first_key, shape, 0, MESH_DEV, dtype=jnp.int32)
    second = jax.random.randint(second_key, shape, 0, MESH_DEV, dtype=jnp.int32)
    return ((band_ids * SECTORS + sector_ids) * MESH_DEV + jnp.minimum(first, second)).astype(jnp.int32)


def draw_edge_counts(key, part):
    band_ids = jnp.arange(BANDS, dtype=jnp.int32)[:, None]
    sector_ids = jnp.arange(SECTORS, dtype=jnp.int32)[None, :]
    distance = jnp.abs(2 * band_ids + 1 - BANDS)
    base = EDGE_DEV // 8 + (EDGE_DEV - EDGE_DEV // 8) * (distance - 1) * (distance - 1) // ((BANDS - 2) * (BANDS - 2))
    jitter_key, pick_key = jax.random.split(jax.random.fold_in(key, 37))
    jitter = jax.random.randint(jitter_key, (BANDS, SECTORS), 0, EDGE_DEV // 64 + 1, dtype=jnp.int32)
    chosen = jax.random.randint(pick_key, (BANDS, 1), 0, SECTORS, dtype=jnp.int32)
    jitter = jnp.where((distance == BANDS - 1) & (sector_ids == chosen), 0, jitter)
    return (base - jitter).astype(jnp.int32)


def steps_of(rng, dims, shards, smallest, top_value):
    loudness = 1.0
    for dim, blocks in shards:
        steps = jax.random.uniform(jax.random.fold_in(jax.random.fold_in(rng, 6), dim), (blocks,), jnp.float32, smallest / len(shards), top_value / len(shards))
        loudness = loudness * jnp.repeat(jnp.exp(steps), dims[dim] // blocks).reshape((-1,) + (1,) * (len(dims) - 1 - dim))
    return loudness


def normal_values(stream_key, dims, width, reach, cuts=(), kind=jnp.bfloat16):
    values = width * jax.random.normal(stream_key, dims, jnp.float32)
    if cuts:
        values = values * steps_of(stream_key, dims, cuts, -0.22, 0.18)
    return jnp.clip(values, -reach, reach).astype(kind)


def setup_inputs(seed: int = 0) -> dict:
    keys = jax.random.split(jax.random.key(seed), 16)
    return {
        "grid_inputs": normal_values(keys[0], (CHANNELS, NLAT, NLON), 1.0, 6.0, ((1, 8), (2, 8))),
        "embed_w1": normal_values(keys[1], (LATENT, CHANNELS), CHANNELS ** -0.5, 0.4375),
        "embed_b1": normal_values(keys[2], (LATENT,), 0.5, 3.0, (), jnp.float32),
        "embed_w2": normal_values(keys[3], (LATENT, LATENT), LATENT ** -0.5, 0.25),
        "embed_gain": jnp.clip(1.0 + 0.18 * jax.random.normal(keys[4], (LATENT,), jnp.float32), 0.1, 1.9),
        "edge_w1": normal_values(keys[5], (LATENT, 3 * LATENT), (3 * LATENT) ** -0.5, 0.15625),
        "edge_b1": normal_values(keys[6], (LATENT,), 0.5, 3.0, (), jnp.float32),
        "edge_w2": normal_values(keys[7], (LATENT, LATENT), LATENT ** -0.5, 0.25),
        "message_gain": jnp.clip(1.0 + 0.18 * jax.random.normal(keys[8], (LATENT,), jnp.float32), 0.1, 1.9),
        "message_bias": normal_values(keys[9], (LATENT,), 0.5, 3.0, (), jnp.float32),
        "mesh_latent": normal_values(keys[10], (LATENT, BANDS, SECTORS, MESH_DEV), 1.0, 6.0, ((0, 4), (1, 8), (2, 8))),
        "edge_latent": normal_values(keys[11], (LATENT, BANDS, SECTORS, EDGE_DEV), 1.0, 6.0, ((0, 4), (1, 8), (2, 8))),
        "senders": draw_senders(jax.random.fold_in(keys[15], 71), 0),
        "receivers": draw_receivers(jax.random.fold_in(keys[15], 71), 0),
        "edge_counts": draw_edge_counts(jax.random.fold_in(keys[15], 71), 0),
    }


epsilon = 1e-05

def normalize(values):
    average = lax.optimization_barrier(jnp.mean(values, axis=0, keepdims=True))
    centred = values - average
    spread = lax.optimization_barrier(jnp.mean(centred * centred, axis=0, keepdims=True))
    return centred * lax.rsqrt(spread + epsilon)

def reference(grid_inputs, embed_w1, embed_b1, embed_w2, embed_gain, edge_w1, edge_b1, edge_w2, message_gain, message_bias, mesh_latent, edge_latent, senders, receivers, edge_counts):
    band_inputs = grid_inputs.reshape(CHANNELS, BANDS, GLAT * NLON).transpose(1, 0, 2)

    def embed_band(block_inputs):
        hidden = jax.nn.silu(jnp.dot(embed_w1, block_inputs, preferred_element_type=jnp.float32) + embed_b1[:, None]).astype(jnp.bfloat16)
        first_pre = jnp.dot(embed_w2, hidden, preferred_element_type=jnp.float32)
        return (normalize(first_pre) * embed_gain[:, None]).astype(jnp.bfloat16)
    band_latent = lax.map(embed_band, band_inputs)
    grid_latent = band_latent.transpose(1, 0, 2).reshape(LATENT, NLAT * NLON)
    tile_count = BANDS * SECTORS
    node_total = tile_count * MESH_DEV
    mesh_flat = mesh_latent.reshape(LATENT, node_total)
    edge_tiles = edge_latent.reshape(LATENT, tile_count, EDGE_DEV).transpose(1, 0, 2)
    send_tiles = senders.reshape(tile_count, EDGE_DEV)
    recv_tiles = receivers.reshape(tile_count, EDGE_DEV)
    count_tiles = edge_counts.reshape(tile_count)
    slot_ids = jnp.arange(EDGE_DEV, dtype=jnp.int32)

    def tile_step(running, inputs):
        totals, degree = running
        edge_cols, send_ids, recv_ids, live_count = inputs
        live_mask = slot_ids < live_count
        stacked = jnp.concatenate([edge_cols, jnp.take(grid_latent, send_ids, axis=1), jnp.take(mesh_flat, recv_ids, axis=1)], axis=0)
        hidden = jax.nn.silu(jnp.dot(edge_w1, stacked, preferred_element_type=jnp.float32) + edge_b1[:, None]).astype(jnp.bfloat16)
        second = jnp.dot(edge_w2, hidden, preferred_element_type=jnp.float32)
        message = (edge_cols.astype(jnp.float32) + normalize(second) * message_gain[:, None] + message_bias[:, None]).astype(jnp.bfloat16)
        weights = jnp.where(live_mask[None, :], message.astype(jnp.float32), jnp.float32(0.0))
        totals = totals + jax.ops.segment_sum(weights.T, recv_ids, num_segments=node_total)
        degree = degree + jax.ops.segment_sum(live_mask.astype(jnp.int32), recv_ids, num_segments=node_total)
        return ((totals, degree), None)
    start_state = (jnp.zeros((node_total, LATENT), jnp.float32), jnp.zeros((node_total,), jnp.int32))
    (totals, degree), unused = lax.scan(tile_step, start_state, (edge_tiles, send_tiles, recv_tiles, count_tiles))
    scale = jnp.maximum(degree, 1).astype(jnp.float32)
    result = mesh_flat.astype(jnp.float32) + totals.T / scale[None, :]
    mesh_out = result.astype(jnp.bfloat16).reshape(LATENT, BANDS, SECTORS, MESH_DEV)
    return (mesh_out, grid_latent.reshape(LATENT, NLAT, NLON))
```

```python
import functools

import jax
import jax.numpy as jnp
from jax import lax
from jax.experimental import pallas as pl
from jax.experimental.pallas import tpu as pltpu
from jax.sharding import PartitionSpec as P

HALO = 8
EPS = 1e-05
F32 = jnp.float32
BF16 = jnp.bfloat16
TILE = 512
ROWS = 16
KPAD = 192


def dot(a, b):
    return jnp.dot(a, b, preferred_element_type=F32)


def dot_nt(a, b):
    return lax.dot_general(a, b, (((1,), (1,)), ((), ())), preferred_element_type=F32)


def half_silu(h):
    return (h + h * jnp.tanh(h)).astype(BF16)


def centred(values):
    average = jnp.mean(values, axis=0, keepdims=True)
    c = values - average
    spread = jnp.mean(c * c, axis=0, keepdims=True)
    return c, lax.rsqrt(spread + EPS)


def wide(column, times):
    return jnp.concatenate([column] * times, axis=1)


def kernel(
    sizes,
    x_hbm, w1t_hbm, w2_hbm, ew1_hbm, ew2_hbm,
    b1_ref, gain_ref, eb1_ref, mgain_ref, mbias_ref,
    mesh_hbm, edge_hbm, send_ref, recv_ref, count_ref,
    out_mesh, out_grid,
    x_v, w1t_v, w2_v, w2r_v, ew1_v, ew2_v, e_own, mesh_own, edges, mesh_full,
    north, south, west, east, corner,
    xf, xc, xh, w1f, w1p, cols, sel, strip, gath, outf, ob, tot, tb, tr,
    local, wsend, wrecv, bar_unused,
):
    gx_n, gy_n, gz_n = sizes
    channels, lat_rows, lon_cols = x_hbm.shape
    latent = w2_v.shape[0]
    share = latent // gz_n
    slots = edge_hbm.shape[1]
    mine = slots // gz_n
    nodes = mesh_hbm.shape[1]
    blocks = lat_rows // ROWS
    gx, gy, gz = lax.axis_index("gx"), lax.axis_index("gy"), lax.axis_index("gz")
    up, down = lax.rem(gx + gx_n - 1, gx_n), lax.rem(gx + 1, gx_n)
    left, right = lax.rem(gy + gy_n - 1, gy_n), lax.rem(gy + 1, gy_n)
    peers = [lax.rem(gz + d, gz_n) for d in range(1, gz_n)]

    places = [{"gz": p} for p in peers]
    places += [{"gx": up}, {"gx": down}, {"gy": left}, {"gy": right}]
    places += [{"gx": a, "gy": b} for a in (up, down) for b in (left, right)]
    barrier = pltpu.get_barrier_semaphore()
    for place in places:
        pl.semaphore_signal(barrier, inc=1, device_id=place, device_id_type=pl.DeviceIdType.MESH)

    def own(index, size=share):
        return pl.ds(pl.multiple_of(index * size, 128), size)

    copies = []

    def bring(src, dst):
        copy = pltpu.make_async_copy(src, dst, local.at[len(copies)])
        copy.start()
        copies.append(copy)
        return copy

    x_in = [bring(x_hbm.at[:, pl.ds(i * ROWS, ROWS), :], x_v.at[i]) for i in range(blocks)]
    w1_in = bring(w1t_hbm, w1t_v)
    w2r_in = [
        bring(w2_hbm.at[own(lax.rem(gz + j, gz_n)), :], w2r_v.at[pl.ds(j * share, share), :])
        for j in range(gz_n)
    ]
    w2_in = bring(w2_hbm, w2_v)
    edge_in = bring(edge_hbm.at[:, own(gz, mine)], edges.at[own(gz), :])
    mesh_in = bring(mesh_hbm, mesh_full.at[own(gz), :])
    mown_in = bring(mesh_hbm, mesh_own)
    eown_in = bring(edge_hbm, e_own)
    ew1_in = bring(ew1_hbm, ew1_v)
    ew2_in = bring(ew2_hbm, ew2_v)

    w1_in.wait()
    w1f[...] = jnp.zeros_like(w1f)
    w1f[0:channels, :] = w1t_v[...].astype(F32) * 0.5
    half_b = b1_ref[...] * 0.5
    for k in range(3):
        piece = half_b.astype(BF16).astype(F32)
        w1f[channels + k : channels + k + 1, :] = piece
        half_b = half_b - piece
    w1p[...] = jnp.transpose(w1f[...])[:, :KPAD].astype(BF16)
    for k, ref in enumerate((gain_ref, eb1_ref, mgain_ref, mbias_ref)):
        cols[k] = jnp.transpose(jnp.broadcast_to(ref[...], (128, latent)))
    pad_rows = lax.broadcasted_iota(jnp.int32, ((KPAD - channels) * ROWS, 128), 0)
    pad_values = jnp.where(pad_rows < 3 * ROWS, 1.0, 0.0).astype(F32)
    xf[pl.ds(channels * ROWS, (KPAD - channels) * ROWS), :] = pad_values

    pl.semaphore_wait(barrier, len(places))
    sent = []

    def send(src, dst, place):
        n = len(sent)
        copy = pltpu.make_async_remote_copy(
            src_ref=src, dst_ref=dst, send_sem=wsend.at[n], recv_sem=wrecv.at[n],
            device_id=place, device_id_type=pl.DeviceIdType.MESH,
        )
        copy.start()
        sent.append(copy)
        return copy

    order = [1, 0, 2] if gz_n == 4 else list(range(gz_n - 1))
    mesh_moves = [send(mesh_hbm, mesh_full.at[own(gz), :], {"gz": peers[d]}) for d in order]
    edge_moves = [
        send(edge_hbm.at[:, own(peers[d], mine)], edges.at[own(gz), :], {"gz": peers[d]})
        for d in order
    ]
    row_moves = [
        send(x_hbm.at[:, pl.ds(0, HALO), :], south, {"gx": up}),
        send(x_hbm.at[:, pl.ds(lat_rows - HALO, HALO), :], north, {"gx": down}),
    ]

    sub = TILE // lon_cols
    for q in range(ROWS // sub):
        k = lax.broadcasted_iota(jnp.int32, (TILE, 256), 0)
        j = lax.broadcasted_iota(jnp.int32, (TILE, 256), 1)
        side, jj = j >> 7, j & 127
        want = ((jj >> 3) - q * sub) * lon_cols + side * (lon_cols - HALO) + (jj & 7)
        sel[q] = jnp.where(k == want, 1.0, 0.0).astype(BF16)

    per = ROWS // sub

    def relayout(i, carry):
        xf[pl.ds(0, channels * ROWS), :] = x_v[i].astype(F32).reshape(channels * ROWS, lon_cols)
        for l in range(ROWS):
            line = xf[pl.ds(l, KPAD, stride=ROWS), :].astype(BF16)
            xc[i * per + l // sub, :, (l % sub) * lon_cols : (l % sub + 1) * lon_cols] = line
        acc = dot(xc[i * per], sel[0])
        for q in range(1, per):
            acc = acc + dot(xc[i * per + q], sel[q])
        strip[0, i] = acc[:, :128].astype(BF16)
        strip[1, i] = acc[:, 128:].astype(BF16)
        return carry

    for copy in x_in:
        copy.wait()
    lax.fori_loop(0, blocks, relayout, 0)
    side_moves = [
        send(strip.at[0], east, {"gy": left}),
        send(strip.at[1], west, {"gy": right}),
        send(strip.at[1, blocks - 1], corner.at[0], {"gx": down, "gy": right}),
        send(strip.at[0, blocks - 1], corner.at[1], {"gx": down, "gy": left}),
        send(strip.at[1, 0], corner.at[2], {"gx": up, "gy": right}),
        send(strip.at[0, 0], corner.at[3], {"gx": up, "gy": left}),
    ]

    sender = send_ref[:, own(gz, mine)]
    lon_total = gy_n * lon_cols
    rl = sender // lon_total - gx * lat_rows + HALO
    cl = sender % lon_total - gy * lon_cols + HALO + lon_total
    cl = cl % lon_total
    cells = lat_rows * lon_cols
    base_n, base_s = cells, cells + HALO * lon_cols
    base_w = cells + 2 * HALO * lon_cols
    base_e = base_w + HALO * lat_rows
    base_c = base_e + HALO * lat_rows
    is_n, is_s = rl < HALO, rl >= lat_rows + HALO
    is_w, is_e = cl < HALO, cl >= lon_cols + HALO
    c_in = jnp.where(is_w, cl, cl - (lon_cols + HALO))
    middle = jnp.where(
        is_n, base_n + rl * lon_cols,
        jnp.where(is_s, base_s + (rl - lat_rows - HALO) * lon_cols, (rl - HALO) * lon_cols),
    ) + cl - HALO
    aside = jnp.where(is_w, base_w, base_e) + (rl - HALO) * HALO + c_in
    cornered = (
        base_c
        + jnp.where(is_n, 0, 2 * 128)
        + jnp.where(is_w, 0, 128)
        + jnp.where(is_n, (rl + ROWS - HALO) * HALO, (rl - lat_rows - HALO) * HALO)
        + c_in
    )
    place_of = jnp.where(is_w | is_e, jnp.where(is_n | is_s, cornered, aside), middle)

    def onehot(base, size):
        ids = lax.broadcasted_iota(jnp.int32, (size, mine), 0)
        return jnp.where(ids == place_of - base, 1.0, 0.0).astype(BF16)

    for copy in w2r_in:
        copy.wait()
    gath[...] = jnp.zeros_like(gath)
    gain_own = cols[0, own(gz), :]

    def embed(i, carry):
        def step(q, inner):
            t = i * per + q
            xt = xc[t]
            hidden = half_silu(dot(w1p[...], xt))
            c, inv = centred(dot(w2r_v[...], hidden))
            out = c[:share] * inv * wide(gain_own, sub)
            for l in range(sub):
                outf[pl.ds(q * sub + l, share, stride=ROWS), :] = out[:, l * lon_cols : (l + 1) * lon_cols]
            gath[...] += dot(xt, onehot(t * TILE, TILE))
            return inner

        lax.fori_loop(0, per, step, 0)
        ob[i] = outf[...].reshape(share, ROWS, lon_cols).astype(BF16)
        pltpu.make_async_copy(ob.at[i], out_grid.at[:, pl.ds(i * ROWS, ROWS), :], bar_unused.at[i]).start()
        return carry

    lax.fori_loop(0, blocks, embed, 0)

    live = count_ref[0, 0]
    tile = gx * gy_n + gy
    node_ids = lax.broadcasted_iota(jnp.int32, (nodes, slots), 0)
    slot_ids = lax.broadcasted_iota(jnp.int32, (nodes, slots), 1)
    near = recv_ref[...] - tile * nodes
    pick = jnp.where((node_ids == near) & (slot_ids < live), 1.0, 0.0).astype(BF16)
    eown_in.wait()
    edge_sum = dot_nt(e_own[...], pick)
    degree = dot_nt(jnp.ones((8, slots), BF16), pick)[0:1, :]
    my_near = recv_ref[:, own(gz, mine)] - tile * nodes
    my_ids = lax.broadcasted_iota(jnp.int32, (nodes, mine), 0)
    my_slots = lax.broadcasted_iota(jnp.int32, (nodes, mine), 1) + gz * mine
    my_pick = jnp.where((my_ids == my_near) & (my_slots < live), 1.0, 0.0).astype(BF16)

    for copy in row_moves:
        copy.wait()
    half = KPAD * HALO
    xf[pl.ds(channels * HALO, (KPAD - channels) * HALO), :] = pad_values[0 : (KPAD - channels) * HALO] * 0.0 + jnp.where(
        lax.broadcasted_iota(jnp.int32, ((KPAD - channels) * HALO, 128), 0) < 3 * HALO, 1.0, 0.0
    ).astype(F32)
    for n, ref in enumerate((north, south)):
        xf[pl.ds(0, channels * HALO), :] = ref[...].astype(F32).reshape(channels * HALO, lon_cols)
        for l in range(HALO):
            xh[n, :, l * lon_cols : (l + 1) * lon_cols] = xf[pl.ds(l, KPAD, stride=HALO), :].astype(BF16)
    acc = gath[...]
    wing = HALO * lon_cols
    acc = acc + dot(xh[0], onehot(base_n, wing)) + dot(xh[1], onehot(base_s, wing))
    for copy in side_moves:
        copy.wait()
    for i in range(blocks):
        acc = acc + dot(west[i], onehot(base_w + i * 128, 128)) + dot(east[i], onehot(base_e + i * 128, 128))
    for i in range(4):
        acc = acc + dot(corner[i], onehot(base_c + i * 128, 128))
    picked = acc.astype(BF16)

    w2_in.wait()
    c, inv = centred(dot(w2_v[...], half_silu(dot(w1p[...], picked))))
    sender_latent = (c * inv * wide(cols[0], mine // 128)).astype(BF16)

    ew1_in.wait()
    mesh_in.wait()
    for copy in mesh_moves:
        copy.wait()
    mesh_cols = dot(mesh_full[...], my_pick).astype(BF16)
    pre = dot(ew1_v[:, latent : 2 * latent], sender_latent) + dot(ew1_v[:, 2 * latent :], mesh_cols)
    edge_in.wait()
    for copy in edge_moves:
        copy.wait()
    pre = pre + dot(ew1_v[:, :latent], edges[...])
    hidden = half_silu((pre + wide(cols[1], mine // 128)) * 0.5)
    ew2_in.wait()
    c, inv = centred(dot(ew2_v[...], hidden))
    tot[...] = dot_nt((c * inv).astype(BF16), my_pick)
    for k in range(gz_n):
        tb[k] = tot[k * share : (k + 1) * share, :].astype(BF16)
    sum_moves = [send(tb.at[peers[d]], tr.at[d], {"gz": peers[d]}) for d in order]
    total = tot[own(gz), :]
    scale = 1.0 / jnp.maximum(degree, 1.0)
    bias_own = wide(cols[3, own(gz), :], nodes // 128)
    gain_m = wide(cols[2, own(gz), :], nodes // 128)
    mown_in.wait()
    known = edge_sum + bias_own * degree
    base = mesh_own[...].astype(F32)
    for copy in sum_moves:
        copy.wait()
    for d in range(gz_n - 1):
        total = total + tr[d].astype(F32)
    out_mesh[...] = (base + (known + gain_m * total) * scale).astype(BF16)
    for i in range(blocks):
        pltpu.make_async_copy(ob.at[i], out_grid.at[:, pl.ds(i * ROWS, ROWS), :], bar_unused.at[i]).wait()


def on_device(
    sizes, grid_inputs, embed_w1, embed_b1, embed_w2, embed_gain, edge_w1, edge_b1, edge_w2,
    message_gain, message_bias, mesh_latent, edge_latent, senders, receivers, edge_counts,
):
    channels, lat_rows, lon_cols = grid_inputs.shape
    latent = embed_w2.shape[0]
    share, nodes, slots = mesh_latent.shape[0], mesh_latent.shape[3], edge_latent.shape[3]
    gz_n = sizes[2]
    mine = slots // gz_n
    blocks = lat_rows // ROWS
    tiles = lat_rows * lon_cols // TILE
    per = blocks and tiles // blocks
    anyspace = pl.BlockSpec(memory_space=pl.ANY)
    vmem = pl.BlockSpec(memory_space=pltpu.VMEM)
    smem = pl.BlockSpec(memory_space=pltpu.SMEM)
    V = pltpu.VMEM
    n_local = blocks + 1 + gz_n + 7
    n_wire = 3 * (gz_n - 1) + 8
    mesh_out, grid_out = pl.pallas_call(
        functools.partial(kernel, sizes),
        out_shape=(
            jax.ShapeDtypeStruct((share, nodes), BF16),
            jax.ShapeDtypeStruct((share, lat_rows, lon_cols), BF16),
        ),
        in_specs=[anyspace] * 5 + [vmem] * 5 + [anyspace] * 2 + [vmem] * 2 + [smem],
        out_specs=(vmem, anyspace),
        scratch_shapes=[
            V((blocks, channels, ROWS, lon_cols), BF16),
            V((channels, latent), BF16),
            V((latent, latent), BF16),
            V((latent, latent), BF16),
            V((latent, 3 * latent), BF16),
            V((latent, latent), BF16),
            V((share, slots), BF16),
            V((share, nodes), BF16),
            V((latent, mine), BF16),
            V((latent, nodes), BF16),
            V((channels, HALO, lon_cols), BF16),
            V((channels, HALO, lon_cols), BF16),
            V((blocks, KPAD, 128), BF16),
            V((blocks, KPAD, 128), BF16),
            V((4, KPAD, 128), BF16),
            V((KPAD * ROWS, lon_cols), F32),
            V((tiles, KPAD, TILE), BF16),
            V((2, KPAD, HALO * lon_cols), BF16),
            V((256, latent), F32),
            V((latent, KPAD), BF16),
            V((4, latent, 128), F32),
            V((per, TILE, 256), BF16),
            V((2, blocks, KPAD, 128), BF16),
            V((KPAD, mine), F32),
            V((share * ROWS, lon_cols), F32),
            V((blocks, share, ROWS, lon_cols), BF16),
            V((latent, nodes), F32),
            V((gz_n, share, nodes), BF16),
            V((gz_n - 1, share, nodes), BF16),
            pltpu.SemaphoreType.DMA((n_local,)),
            pltpu.SemaphoreType.DMA((n_wire,)),
            pltpu.SemaphoreType.DMA((n_wire,)),
            pltpu.SemaphoreType.DMA((blocks,)),
        ],
        compiler_params=pltpu.CompilerParams(
            collective_id=0, has_side_effects=True, vmem_limit_bytes=56 * 1024 * 1024
        ),
    )(
        grid_inputs, embed_w1.T, embed_w2, edge_w1, edge_w2,
        embed_b1.reshape(1, latent), embed_gain.reshape(1, latent), edge_b1.reshape(1, latent),
        message_gain.reshape(1, latent), message_bias.reshape(1, latent),
        mesh_latent.reshape(share, nodes), edge_latent.reshape(share, slots),
        senders.reshape(1, slots), receivers.reshape(1, slots), edge_counts,
    )
    return mesh_out.reshape(share, 1, 1, nodes), grid_out


def solution(mesh):
    sizes = (mesh.shape["gx"], mesh.shape["gy"], mesh.shape["gz"])
    return jax.shard_map(
        functools.partial(on_device, sizes),
        mesh=mesh,
        in_specs=(
            P(None, "gx", "gy"), P(), P(), P(), P(), P(), P(), P(), P(), P(),
            P("gz", "gx", "gy", None), P("gz", "gx", "gy", None),
            P("gx", "gy", None), P("gx", "gy", None), P("gx", "gy"),
        ),
        out_specs=(P("gz", "gx", "gy", None), P("gz", "gx", "gy")),
        check_vma=False,
    )
```

```python
import functools

import jax
import jax.numpy as jnp
from jax import lax
from jax.experimental import pallas as pl
from jax.experimental.pallas import tpu as pltpu
from jax.sharding import PartitionSpec as P

HALO = 8
EPS = 1e-05
FILL = (2, 4, 4, 7)
F32 = jnp.float32
BF16 = jnp.bfloat16
TILE = 512
PARTS = 2
ROWS = 16
KPAD = 192


def dot(a, b):
    return jnp.dot(a, b, preferred_element_type=F32)


def dot_nt(a, b):
    return lax.dot_general(a, b, (((1,), (1,)), ((), ())), preferred_element_type=F32)


def half_silu(h):
    return (h + h * jnp.tanh(h)).astype(BF16)


def centred(values):
    average = jnp.mean(values, axis=0, keepdims=True)
    c = values - average
    spread = jnp.mean(c * c, axis=0, keepdims=True)
    return c, lax.rsqrt(spread + EPS)


def wide(column, times):
    return jnp.concatenate([column] * times, axis=1)


def kernel(
    sizes,
    x_hbm, w1t_hbm, w2_hbm, ew1_hbm, ew2_hbm,
    b1_ref, gain_ref, eb1_ref, mgain_ref, mbias_ref,
    mesh_hbm, edge_hbm, send_ref, recv_ref, count_ref,
    out_mesh, out_blocks,
    x_v, w1t_v, w2_v, w2r_v, ew1_v, ew2_v, e_own, mesh_own, edges, mesh_full,
    north, south, west, east, corner,
    xf, xc, xh, w1f, w1p, cols, sel, strip, gath, outf, ob, tot, tb, tr,
    hid_a, hid_b, pre_s, pick_s,
    local, wsend, wrecv, leave,
):
    gx_n, gy_n, gz_n = sizes
    channels, lat_rows, lon_cols = x_hbm.shape
    latent = w2_v.shape[0]
    share = latent // gz_n
    slots = edge_hbm.shape[1]
    mine = slots // gz_n
    nodes = mesh_hbm.shape[1]
    blocks = lat_rows // ROWS
    gx, gy, gz = lax.axis_index("gx"), lax.axis_index("gy"), lax.axis_index("gz")
    up, down = lax.rem(gx + gx_n - 1, gx_n), lax.rem(gx + 1, gx_n)
    left, right = lax.rem(gy + gy_n - 1, gy_n), lax.rem(gy + 1, gy_n)
    peers = [lax.rem(gz + d, gz_n) for d in range(1, gz_n)]

    places = [{"gz": p} for p in peers]
    places += [{"gx": up}, {"gx": down}, {"gy": left}, {"gy": right}]
    y, z_lo = lax.rem(gy, 4), gy // 4
    lean_e = jnp.where(y == 3, jnp.where(z_lo == 0, gz_n - 1, 1), 0)
    lean_w = jnp.where(y == 0, jnp.where(z_lo == 0, gz_n - 1, 1), 0)
    east_place = {"gy": right, "gz": lax.rem(gz + lean_e, gz_n)}
    west_place = {"gy": left, "gz": lax.rem(gz + lean_w, gz_n)}
    places += [east_place, west_place]
    barrier = pltpu.get_barrier_semaphore()
    for place in places:
        pl.semaphore_signal(barrier, inc=1, device_id=place, device_id_type=pl.DeviceIdType.MESH)

    def own(index, size=share):
        return pl.ds(pl.multiple_of(index * size, 128), size)

    copies = []

    def bring(src, dst):
        copy = pltpu.make_async_copy(src, dst, local.at[len(copies)])
        copy.start()
        copies.append(copy)
        return copy

    x_in = [bring(x_hbm.at[:, pl.ds(i * ROWS, ROWS), :], x_v.at[i]) for i in range(blocks)]
    w1_in = bring(w1t_hbm, w1t_v)
    w2r_in = [
        bring(w2_hbm.at[own(lax.rem(gz + j, gz_n)), :], w2r_v.at[pl.ds(j * share, share), :])
        for j in range(gz_n)
    ]
    w2_in = bring(w2_hbm, w2_v)
    part = mine // PARTS
    edge_in = [
        bring(edge_hbm.at[:, own(gz * PARTS + b, part)], edges.at[b, own(gz), :]) for b in range(PARTS)
    ]
    mesh_in = bring(mesh_hbm, mesh_full.at[own(gz), :])
    mown_in = bring(mesh_hbm, mesh_own)
    eown_in = bring(edge_hbm, e_own)
    ew1_in = bring(ew1_hbm, ew1_v)
    ew2_in = bring(ew2_hbm, ew2_v)

    w1_in.wait()
    w1f[...] = jnp.zeros_like(w1f)
    w1f[0:channels, :] = w1t_v[...].astype(F32) * 0.5
    half_b = b1_ref[...] * 0.5
    for k in range(3):
        piece = half_b.astype(BF16).astype(F32)
        w1f[channels + k : channels + k + 1, :] = piece
        half_b = half_b - piece
    w1p[...] = jnp.transpose(w1f[...])[:, :KPAD].astype(BF16)
    for k, ref in enumerate((gain_ref, eb1_ref, mgain_ref, mbias_ref)):
        cols[k] = jnp.transpose(jnp.broadcast_to(ref[...], (128, latent)))
    pad_rows = lax.broadcasted_iota(jnp.int32, ((KPAD - channels) * ROWS, 128), 0)
    pad_values = jnp.where(pad_rows < 3 * ROWS, 1.0, 0.0).astype(F32)
    xf[pl.ds(channels * ROWS, (KPAD - channels) * ROWS), :] = pad_values

    pl.semaphore_wait(barrier, len(places))
    sent = []

    def send(src, dst, place):
        n = len(sent)
        copy = pltpu.make_async_remote_copy(
            src_ref=src, dst_ref=dst, send_sem=wsend.at[n], recv_sem=wrecv.at[n],
            device_id=place, device_id_type=pl.DeviceIdType.MESH,
        )
        copy.start()
        sent.append(copy)
        return copy

    order = [1, 0, 2] if gz_n == 4 else list(range(gz_n - 1))
    mesh_moves = [send(mesh_hbm, mesh_full.at[own(gz), :], {"gz": peers[d]}) for d in order]
    row_moves = [
        send(x_hbm.at[:, pl.ds(0, HALO), :], south, {"gx": up}),
        send(x_hbm.at[:, pl.ds(lat_rows - HALO, HALO), :], north, {"gx": down}),
    ]
    sub = TILE // lon_cols
    for q in range(ROWS // sub):
        k = lax.broadcasted_iota(jnp.int32, (TILE, 256), 0)
        j = lax.broadcasted_iota(jnp.int32, (TILE, 256), 1)
        side, jj = j >> 7, j & 127
        want = ((jj >> 3) - q * sub) * lon_cols + side * (lon_cols - HALO) + (jj & 7)
        sel[q] = jnp.where(k == want, 1.0, 0.0).astype(BF16)

    per = ROWS // sub

    def relayout(i, carry):
        xf[pl.ds(0, channels * ROWS), :] = x_v[i].astype(F32).reshape(channels * ROWS, lon_cols)
        for l in range(ROWS):
            line = xf[pl.ds(l, KPAD, stride=ROWS), :].astype(BF16)
            xc[i * per + l // sub, :, (l % sub) * lon_cols : (l % sub + 1) * lon_cols] = line
        acc = dot(xc[i * per], sel[0])
        for q in range(1, per):
            acc = acc + dot(xc[i * per + q], sel[q])
        strip[0, i] = acc[:, :128].astype(BF16)
        strip[1, i] = acc[:, 128:].astype(BF16)
        return carry

    for copy in x_in:
        copy.wait()
    lax.fori_loop(0, blocks, relayout, 0)
    cut = blocks // 2
    side_moves = [
        send(strip.at[0, pl.ds(0, cut)], east.at[pl.ds(0, cut)], {"gy": left}),
        send(strip.at[1, pl.ds(0, cut)], west.at[pl.ds(0, cut)], {"gy": right}),
        send(strip.at[0, pl.ds(cut, cut)], east.at[pl.ds(cut, cut)], west_place),
        send(strip.at[1, pl.ds(cut, cut)], west.at[pl.ds(cut, cut)], east_place),
    ]
    edge_moves = [
        [
            send(edge_hbm.at[:, own(peers[d] * PARTS + b, part)], edges.at[b, own(gz), :], {"gz": peers[d]})
            for d in order
        ]
        for b in range(PARTS)
    ]

    sender = send_ref[:, own(gz, mine)]
    lon_total = gy_n * lon_cols
    rl = sender // lon_total - gx * lat_rows + HALO
    cl = sender % lon_total - gy * lon_cols + HALO + lon_total
    cl = cl % lon_total
    cells = lat_rows * lon_cols
    base_n, base_s = cells, cells + HALO * lon_cols
    base_w = cells + 2 * HALO * lon_cols
    base_e = base_w + HALO * lat_rows
    base_c = base_e + HALO * lat_rows
    is_n, is_s = rl < HALO, rl >= lat_rows + HALO
    is_w, is_e = cl < HALO, cl >= lon_cols + HALO
    c_in = jnp.where(is_w, cl, cl - (lon_cols + HALO))
    middle = jnp.where(
        is_n, base_n + rl * lon_cols,
        jnp.where(is_s, base_s + (rl - lat_rows - HALO) * lon_cols, (rl - HALO) * lon_cols),
    ) + cl - HALO
    aside = jnp.where(is_w, base_w, base_e) + (rl - HALO) * HALO + c_in
    cornered = (
        base_c
        + jnp.where(is_n, 0, 2 * 128)
        + jnp.where(is_w, 0, 128)
        + jnp.where(is_n, (rl + ROWS - HALO) * HALO, (rl - lat_rows - HALO) * HALO)
        + c_in
    )
    place_of = jnp.where(is_w | is_e, jnp.where(is_n | is_s, cornered, aside), middle)

    def onehot(base, size):
        ids = lax.broadcasted_iota(jnp.int32, (size, mine), 0)
        return jnp.where(ids == place_of - base, 1.0, 0.0).astype(BF16)

    gath[...] = jnp.zeros_like(gath)

    def gather(t, carry):
        gath[...] += dot(xc[t], onehot(t * TILE, TILE))
        return carry

    tiles = cells // TILE
    lax.fori_loop(0, tiles, gather, 0)

    live = count_ref[0, 0]
    tile = gx * gy_n + gy
    for b in range(PARTS):
        near = recv_ref[:, own(gz * PARTS + b, part)] - tile * nodes
        ids = lax.broadcasted_iota(jnp.int32, (nodes, part), 0)
        spots = lax.broadcasted_iota(jnp.int32, (nodes, part), 1) + (gz * PARTS + b) * part
        pick_s[b] = jnp.where((ids == near) & (spots < live), 1.0, 0.0).astype(BF16)

    for copy in w2r_in:
        copy.wait()
    gain_own = cols[0, own(gz), :]
    first = latent // 2

    def layers(t_in, hid_out, hid_in, spot):
        pieces = []
        for r in range(2):
            rows = slice(r * first, (r + 1) * first)
            h = dot(w1p[rows, :], xc[t_in])
            pieces.append(dot(w2r_v[rows, :], hid_in[...]))
            hid_out[rows, :] = half_silu(h)
            if r == 0:
                shift = jnp.mean(pieces[0], axis=0, keepdims=True)
                d = pieces[0] - shift
                d_own = d[:share]
                squares = jnp.sum(d * d, axis=0, keepdims=True)
            else:
                d = pieces[1] - shift
                lean = jnp.sum(d, axis=0, keepdims=True) * (1.0 / latent)
                squares = squares + jnp.sum(d * d, axis=0, keepdims=True)
        spread = squares * (1.0 / latent) - lean * lean
        out = (d_own - lean) * lax.rsqrt(spread + EPS) * wide(gain_own, sub)
        for l in range(sub):
            outf[pl.ds(spot * sub + l, share, stride=2 * sub), :] = out[:, l * lon_cols : (l + 1) * lon_cols]

    def leaving(u):
        return pltpu.make_async_copy(ob.at[u], out_blocks.at[u], leave.at[u])

    def pair(u, carry):
        layers(2 * u + 1, hid_b, hid_a, 0)
        layers(jnp.minimum(2 * u + 2, tiles - 1), hid_a, hid_b, 1)
        ob[u] = outf[...].reshape(share, 2 * sub, lon_cols).astype(BF16)
        leaving(u).start()
        return carry

    def embed(start, stop):
        lax.fori_loop(start, stop, pair, 0)

    hid_a[...] = half_silu(dot(w1p[...], xc[0]))
    stops = FILL + (tiles // 2,)
    embed(0, stops[0])
    for copy in side_moves:
        copy.wait()
    corner_moves = [
        send(west.at[blocks - 1], corner.at[0], {"gx": down}),
        send(east.at[blocks - 1], corner.at[1], {"gx": down}),
        send(west.at[0], corner.at[2], {"gx": up}),
        send(east.at[0], corner.at[3], {"gx": up}),
    ]

    for copy in row_moves:
        copy.wait()
    half = KPAD * HALO
    xf[pl.ds(channels * HALO, (KPAD - channels) * HALO), :] = pad_values[0 : (KPAD - channels) * HALO] * 0.0 + jnp.where(
        lax.broadcasted_iota(jnp.int32, ((KPAD - channels) * HALO, 128), 0) < 3 * HALO, 1.0, 0.0
    ).astype(F32)
    for n, ref in enumerate((north, south)):
        xf[pl.ds(0, channels * HALO), :] = ref[...].astype(F32).reshape(channels * HALO, lon_cols)
        for l in range(HALO):
            xh[n, :, l * lon_cols : (l + 1) * lon_cols] = xf[pl.ds(l, KPAD, stride=HALO), :].astype(BF16)
    acc = gath[...]
    wing = HALO * lon_cols
    acc = acc + dot(xh[0], onehot(base_n, wing)) + dot(xh[1], onehot(base_s, wing))
    for i in range(blocks):
        acc = acc + dot(west[i], onehot(base_w + i * 128, 128)) + dot(east[i], onehot(base_e + i * 128, 128))
    gath[...] = acc
    embed(stops[0], stops[1])
    for copy in corner_moves:
        copy.wait()
    acc = gath[...]
    for i in range(4):
        acc = acc + dot(corner[i], onehot(base_c + i * 128, 128))
    picked = acc.astype(BF16)

    w2_in.wait()
    c, inv = centred(dot(w2_v[...], half_silu(dot(w1p[...], picked))))
    sender_latent = (c * inv * wide(cols[0], mine // 128)).astype(BF16)
    ew1_in.wait()
    for b in range(PARTS):
        pre_s[b] = dot(ew1_v[:, latent : 2 * latent], sender_latent[:, b * part : (b + 1) * part]) + wide(
            cols[1], part // 128
        )

    def edge_net(b):
        edge_in[b].wait()
        for copy in edge_moves[b]:
            copy.wait()
        pre = pre_s[b] + dot(ew1_v[:, :latent], edges[b])
        c, inv = centred(dot(ew2_v[...], half_silu(pre * 0.5)))
        part_sum = dot_nt((c * inv).astype(BF16), pick_s[b])
        tot[...] = part_sum if b == 0 else tot[...] + part_sum

    mesh_in.wait()
    for copy in mesh_moves:
        copy.wait()
    for b in range(PARTS):
        mesh_cols = dot(mesh_full[...], pick_s[b]).astype(BF16)
        pre_s[b] += dot(ew1_v[:, 2 * latent :], mesh_cols)
    ew2_in.wait()
    for b in range(PARTS):
        embed(stops[b + 1], stops[b + 2])
        edge_net(b)
    for k in range(gz_n):
        tb[k] = tot[k * share : (k + 1) * share, :].astype(BF16)
    sum_moves = [send(tb.at[peers[d]], tr.at[d], {"gz": peers[d]}) for d in order]

    embed(stops[PARTS + 1], stops[PARTS + 2])
    node_ids = lax.broadcasted_iota(jnp.int32, (nodes, slots), 0)
    slot_ids = lax.broadcasted_iota(jnp.int32, (nodes, slots), 1)
    pick = jnp.where((node_ids == recv_ref[...] - tile * nodes) & (slot_ids < live), 1.0, 0.0).astype(BF16)
    eown_in.wait()
    edge_sum = dot_nt(e_own[...], pick)
    degree = dot_nt(jnp.ones((8, slots), BF16), pick)[0:1, :]
    scale = 1.0 / jnp.maximum(degree, 1.0)
    gain_m = wide(cols[2, own(gz), :], nodes // 128)
    known = edge_sum + wide(cols[3, own(gz), :], nodes // 128) * degree
    mown_in.wait()
    total = tot[own(gz), :]
    for copy in sum_moves:
        copy.wait()
    for d in range(gz_n - 1):
        total = total + tr[d].astype(F32)
    out_mesh[...] = (mesh_own[...].astype(F32) + (known + gain_m * total) * scale).astype(BF16)
    for u in range(tiles // 2):
        leaving(u).wait()


def deliver(mesh_ref, blocks_hbm, out_mesh, out_grid, buf, sin, sout):
    count, _, rows, _ = blocks_hbm.shape
    ins = [pltpu.make_async_copy(blocks_hbm.at[u], buf.at[u], sin.at[u]) for u in range(count)]
    outs = [
        pltpu.make_async_copy(buf.at[u], out_grid.at[:, pl.ds(u * rows, rows), :], sout.at[u])
        for u in range(count)
    ]
    for copy in ins:
        copy.start()
    out_mesh[...] = mesh_ref[...]
    for came, goes in zip(ins, outs):
        came.wait()
        goes.start()
    for copy in outs:
        copy.wait()


def on_device(
    sizes, grid_inputs, embed_w1, embed_b1, embed_w2, embed_gain, edge_w1, edge_b1, edge_w2,
    message_gain, message_bias, mesh_latent, edge_latent, senders, receivers, edge_counts,
):
    channels, lat_rows, lon_cols = grid_inputs.shape
    latent = embed_w2.shape[0]
    share, nodes, slots = mesh_latent.shape[0], mesh_latent.shape[3], edge_latent.shape[3]
    gz_n = sizes[2]
    mine = slots // gz_n
    blocks = lat_rows // ROWS
    tiles = lat_rows * lon_cols // TILE
    per = blocks and tiles // blocks
    anyspace = pl.BlockSpec(memory_space=pl.ANY)
    vmem = pl.BlockSpec(memory_space=pltpu.VMEM)
    smem = pl.BlockSpec(memory_space=pltpu.SMEM)
    V = pltpu.VMEM
    n_local = blocks + 1 + gz_n + 6 + PARTS
    n_wire = (2 + PARTS) * (gz_n - 1) + 10
    pairs, out_rows = tiles // 2, 2 * TILE // lon_cols
    mesh_out, grid_blocks = pl.pallas_call(
        functools.partial(kernel, sizes),
        out_shape=(
            jax.ShapeDtypeStruct((share, nodes), BF16),
            jax.ShapeDtypeStruct((pairs, share, out_rows, lon_cols), BF16),
        ),
        in_specs=[anyspace] * 5 + [vmem] * 5 + [anyspace] * 2 + [vmem] * 2 + [smem],
        out_specs=(vmem, anyspace),
        scratch_shapes=[
            V((blocks, channels, ROWS, lon_cols), BF16),
            V((channels, latent), BF16),
            V((latent, latent), BF16),
            V((latent, latent), BF16),
            V((latent, 3 * latent), BF16),
            V((latent, latent), BF16),
            V((share, slots), BF16),
            V((share, nodes), BF16),
            V((PARTS, latent, mine // PARTS), BF16),
            V((latent, nodes), BF16),
            V((channels, HALO, lon_cols), BF16),
            V((channels, HALO, lon_cols), BF16),
            V((blocks, KPAD, 128), BF16),
            V((blocks, KPAD, 128), BF16),
            V((4, KPAD, 128), BF16),
            V((KPAD * ROWS, lon_cols), F32),
            V((tiles, KPAD, TILE), BF16),
            V((2, KPAD, HALO * lon_cols), BF16),
            V((256, latent), F32),
            V((latent, KPAD), BF16),
            V((4, latent, 128), F32),
            V((per, TILE, 256), BF16),
            V((2, blocks, KPAD, 128), BF16),
            V((KPAD, mine), F32),
            V((share * out_rows, lon_cols), F32),
            V((pairs, share, out_rows, lon_cols), BF16),
            V((latent, nodes), F32),
            V((gz_n, share, nodes), BF16),
            V((gz_n - 1, share, nodes), BF16),
            V((latent, TILE), BF16),
            V((latent, TILE), BF16),
            V((PARTS, latent, mine // PARTS), F32),
            V((PARTS, nodes, mine // PARTS), BF16),
            pltpu.SemaphoreType.DMA((n_local,)),
            pltpu.SemaphoreType.DMA((n_wire,)),
            pltpu.SemaphoreType.DMA((n_wire,)),
            pltpu.SemaphoreType.DMA((pairs,)),
        ],
        compiler_params=pltpu.CompilerParams(
            collective_id=0, has_side_effects=True, vmem_limit_bytes=56 * 1024 * 1024
        ),
    )(
        grid_inputs, embed_w1.T, embed_w2, edge_w1, edge_w2,
        embed_b1.reshape(1, latent), embed_gain.reshape(1, latent), edge_b1.reshape(1, latent),
        message_gain.reshape(1, latent), message_bias.reshape(1, latent),
        mesh_latent.reshape(share, nodes), edge_latent.reshape(share, slots),
        senders.reshape(1, slots), receivers.reshape(1, slots), edge_counts,
    )
    mesh_out, grid_out = pl.pallas_call(
        deliver,
        out_shape=(
            jax.ShapeDtypeStruct((share, nodes), BF16),
            jax.ShapeDtypeStruct((share, lat_rows, lon_cols), BF16),
        ),
        in_specs=[vmem, anyspace],
        out_specs=(vmem, anyspace),
        scratch_shapes=[
            V((pairs, share, out_rows, lon_cols), BF16),
            pltpu.SemaphoreType.DMA((pairs,)),
            pltpu.SemaphoreType.DMA((pairs,)),
        ],
    )(mesh_out, grid_blocks)
    return mesh_out.reshape(share, 1, 1, nodes), grid_out


def solution(mesh):
    sizes = (mesh.shape["gx"], mesh.shape["gy"], mesh.shape["gz"])
    return jax.shard_map(
        functools.partial(on_device, sizes),
        mesh=mesh,
        in_specs=(
            P(None, "gx", "gy"), P(), P(), P(), P(), P(), P(), P(), P(), P(),
            P("gz", "gx", "gy", None), P("gz", "gx", "gy", None),
            P("gx", "gy", None), P("gx", "gy", None), P("gx", "gy"),
        ),
        out_specs=(P("gz", "gx", "gy", None), P("gz", "gx", "gy")),
        check_vma=False,
    )
```

```python
import functools

import jax
import jax.numpy as jnp
from jax import lax
from jax.experimental import pallas as pl
from jax.experimental.pallas import tpu as pltpu
from jax.sharding import PartitionSpec as P

HALO = 8
EPS = 1e-05
FILL = (5, 6, 6, 6)
F32 = jnp.float32
BF16 = jnp.bfloat16
TILE = 512
PARTS = 2
ROWS = 16
KPAD = 192


def dot(a, b):
    return jnp.dot(a, b, preferred_element_type=F32)


def dot_nt(a, b):
    return lax.dot_general(a, b, (((1,), (1,)), ((), ())), preferred_element_type=F32)


def half_silu(h):
    return (h + h * jnp.tanh(h)).astype(BF16)


def centred(values):
    average = jnp.mean(values, axis=0, keepdims=True)
    c = values - average
    spread = jnp.mean(c * c, axis=0, keepdims=True)
    return c, lax.rsqrt(spread + EPS)


def wide(column, times):
    return jnp.concatenate([column] * times, axis=1)


def kernel(
    sizes,
    x_hbm, w1t_hbm, w2_hbm, ew1_hbm, ew2_hbm,
    b1_hbm, gain_hbm, eb1_hbm, mgain_hbm, mbias_hbm,
    mesh_hbm, edge_hbm, send_hbm, recv_hbm, count_ref,
    out_mesh, out_blocks,
    x_v, w1t_v, w2_v, w2r_v, ew1_v, ew2_v, e_own, mesh_own, edges, mesh_full,
    north, south, west, east, corner,
    xf, xc, xh, w1f, w1p, cols, sel, strip, gath, outf, tot, tb, tr,
    hid_a, hid_b, pre_s, pick_s,
    vecs, send_ref, recv_ref,
    local, wsend, wrecv,
):
    gx_n, gy_n, gz_n = sizes
    channels, lat_rows, lon_cols = x_hbm.shape
    latent = w2_v.shape[0]
    share = latent // gz_n
    slots = edge_hbm.shape[1]
    mine = slots // gz_n
    nodes = mesh_hbm.shape[1]
    blocks = lat_rows // ROWS
    gx, gy, gz = lax.axis_index("gx"), lax.axis_index("gy"), lax.axis_index("gz")
    up, down = lax.rem(gx + gx_n - 1, gx_n), lax.rem(gx + 1, gx_n)
    left, right = lax.rem(gy + gy_n - 1, gy_n), lax.rem(gy + 1, gy_n)
    peers = [lax.rem(gz + d, gz_n) for d in range(1, gz_n)]

    places = [{"gz": p} for p in peers]
    places += [{"gx": up}, {"gx": down}, {"gy": left}, {"gy": right}]
    y, z_lo = lax.rem(gy, 4), gy // 4
    lean_e = jnp.where(y == 3, jnp.where(z_lo == 0, gz_n - 1, 1), 0)
    lean_w = jnp.where(y == 0, jnp.where(z_lo == 0, gz_n - 1, 1), 0)
    east_place = {"gy": right, "gz": lax.rem(gz + lean_e, gz_n)}
    west_place = {"gy": left, "gz": lax.rem(gz + lean_w, gz_n)}
    places += [east_place, west_place]
    barrier = pltpu.get_barrier_semaphore()
    for place in places:
        pl.semaphore_signal(barrier, inc=1, device_id=place, device_id_type=pl.DeviceIdType.MESH)

    def own(index, size=share):
        return pl.ds(pl.multiple_of(index * size, 128), size)

    vec_hbm = (b1_hbm, gain_hbm, eb1_hbm, mgain_hbm, mbias_hbm)
    copies = []

    def bring(src, dst):
        copy = pltpu.make_async_copy(src, dst, local.at[len(copies)])
        copy.start()
        copies.append(copy)
        return copy

    w1_in = bring(w1t_hbm, w1t_v)
    vec_in = [bring(ref, vecs.at[k]) for k, ref in enumerate(vec_hbm)]
    x_in = [bring(x_hbm.at[:, pl.ds(i * ROWS, ROWS), :], x_v.at[i]) for i in range(blocks)]
    part = mine // PARTS
    pl.semaphore_wait(barrier, len(places))
    sent = []

    def send(src, dst, place):
        n = len(sent)
        copy = pltpu.make_async_remote_copy(
            src_ref=src, dst_ref=dst, send_sem=wsend.at[n], recv_sem=wrecv.at[n],
            device_id=place, device_id_type=pl.DeviceIdType.MESH,
        )
        copy.start()
        sent.append(copy)
        return copy

    after, across, before = peers
    mesh_moves = [send(mesh_hbm, mesh_full.at[own(gz), :], {"gz": p}) for p in (after, before)]

    def send_edges(b, p):
        return send(edge_hbm.at[:, own(p * PARTS + b, part)], edges.at[b, own(gz), :], {"gz": p})

    edge_moves = [[], []]
    row_moves = [
        send(x_hbm.at[:, pl.ds(0, HALO), :], south, {"gx": up}),
        send(x_hbm.at[:, pl.ds(lat_rows - HALO, HALO), :], north, {"gx": down}),
    ]
    w1_in.wait()
    for copy in vec_in:
        copy.wait()
    w1f[...] = jnp.zeros_like(w1f)
    w1f[0:channels, :] = w1t_v[...].astype(F32) * 0.5
    half_b = vecs[0] * 0.5
    for k in range(3):
        piece = half_b.astype(BF16).astype(F32)
        w1f[channels + k : channels + k + 1, :] = piece
        half_b = half_b - piece
    w1p[...] = jnp.transpose(w1f[...])[:, :KPAD].astype(BF16)
    for k in range(4):
        cols[k] = jnp.transpose(jnp.broadcast_to(vecs[k + 1], (128, latent)))
    pad_rows = lax.broadcasted_iota(jnp.int32, ((KPAD - channels) * ROWS, 128), 0)
    pad_values = jnp.where(pad_rows < 3 * ROWS, 1.0, 0.0).astype(F32)
    xf[pl.ds(channels * ROWS, (KPAD - channels) * ROWS), :] = pad_values

    sub = TILE // lon_cols
    for q in range(ROWS // sub):
        k = lax.broadcasted_iota(jnp.int32, (TILE, 256), 0)
        j = lax.broadcasted_iota(jnp.int32, (TILE, 256), 1)
        side, jj = j >> 7, j & 127
        want = ((jj >> 3) - q * sub) * lon_cols + side * (lon_cols - HALO) + (jj & 7)
        sel[q] = jnp.where(k == want, 1.0, 0.0).astype(BF16)

    per = ROWS // sub

    def relayout(i, carry):
        xf[pl.ds(0, channels * ROWS), :] = x_v[i].astype(F32).reshape(channels * ROWS, lon_cols)
        for l in range(ROWS):
            line = xf[pl.ds(l, KPAD, stride=ROWS), :].astype(BF16)
            xc[i * per + l // sub, :, (l % sub) * lon_cols : (l % sub + 1) * lon_cols] = line
        acc = dot(xc[i * per], sel[0])
        for q in range(1, per):
            acc = acc + dot(xc[i * per + q], sel[q])
        strip[0, i] = acc[:, :128].astype(BF16)
        strip[1, i] = acc[:, 128:].astype(BF16)
        return carry

    for copy in x_in:
        copy.wait()
    w2r_in = [
        bring(w2_hbm.at[own(lax.rem(gz + j, gz_n)), :], w2r_v.at[pl.ds(j * share, share), :])
        for j in range(gz_n)
    ]
    w2_in = bring(w2_hbm, w2_v)
    index_in = [bring(send_hbm, send_ref), bring(recv_hbm, recv_ref)]
    edge_in = [
        bring(edge_hbm.at[:, own(gz * PARTS + b, part)], edges.at[b, own(gz), :]) for b in range(PARTS)
    ]
    mesh_in = bring(mesh_hbm, mesh_full.at[own(gz), :])
    mown_in = bring(mesh_hbm, mesh_own)
    eown_in = bring(edge_hbm, e_own)
    ew1_in = bring(ew1_hbm, ew1_v)
    ew2_in = bring(ew2_hbm, ew2_v)

    lax.fori_loop(0, blocks, relayout, 0)
    cut = blocks // 2
    side_moves = [
        send(strip.at[0, pl.ds(0, cut)], east.at[pl.ds(0, cut)], {"gy": left}),
        send(strip.at[1, pl.ds(0, cut)], west.at[pl.ds(0, cut)], {"gy": right}),
        send(strip.at[0, pl.ds(cut, cut)], east.at[pl.ds(cut, cut)], west_place),
        send(strip.at[1, pl.ds(cut, cut)], west.at[pl.ds(cut, cut)], east_place),
    ]
    edge_moves[0] += [send_edges(0, p) for p in (across, after, before)]
    for copy in index_in:
        copy.wait()
    sender = send_ref[:, own(gz, mine)]
    lon_total = gy_n * lon_cols
    rl = sender // lon_total - gx * lat_rows + HALO
    cl = sender % lon_total - gy * lon_cols + HALO + lon_total
    cl = cl % lon_total
    cells = lat_rows * lon_cols
    base_n, base_s = cells, cells + HALO * lon_cols
    base_w = cells + 2 * HALO * lon_cols
    base_e = base_w + HALO * lat_rows
    base_c = base_e + HALO * lat_rows
    is_n, is_s = rl < HALO, rl >= lat_rows + HALO
    is_w, is_e = cl < HALO, cl >= lon_cols + HALO
    c_in = jnp.where(is_w, cl, cl - (lon_cols + HALO))
    middle = jnp.where(
        is_n, base_n + rl * lon_cols,
        jnp.where(is_s, base_s + (rl - lat_rows - HALO) * lon_cols, (rl - HALO) * lon_cols),
    ) + cl - HALO
    aside = jnp.where(is_w, base_w, base_e) + (rl - HALO) * HALO + c_in
    cornered = (
        base_c
        + jnp.where(is_n, 0, 2 * 128)
        + jnp.where(is_w, 0, 128)
        + jnp.where(is_n, (rl + ROWS - HALO) * HALO, (rl - lat_rows - HALO) * HALO)
        + c_in
    )
    place_of = jnp.where(is_w | is_e, jnp.where(is_n | is_s, cornered, aside), middle)

    def onehot(base, size):
        ids = lax.broadcasted_iota(jnp.int32, (size, mine), 0)
        return jnp.where(ids == place_of - base, 1.0, 0.0).astype(BF16)

    gath[...] = jnp.zeros_like(gath)

    def gather(t, carry):
        found = dot(xc[t * per], onehot(t * per * TILE, TILE))
        for q in range(1, per):
            found = found + dot(xc[t * per + q], onehot((t * per + q) * TILE, TILE))
        gath[...] += found
        return carry

    tiles = cells // TILE
    lax.fori_loop(0, blocks, gather, 0)

    for copy in mesh_moves:
        copy.wait()
    upper = mesh_full.at[pl.ds(pl.multiple_of(before * share, 128), share // 2), :]
    lower = mesh_full.at[pl.ds(pl.multiple_of(after * share + share // 2, 64), share // 2), :]
    mesh_moves = [send(upper, upper, {"gz": after}), send(lower, lower, {"gz": before})]
    edge_moves[1] = [send_edges(1, p) for p in (across, after, before)]

    live = count_ref[0, 0]
    tile = gx * gy_n + gy
    for b in range(PARTS):
        near = recv_ref[:, own(gz * PARTS + b, part)] - tile * nodes
        ids = lax.broadcasted_iota(jnp.int32, (nodes, part), 0)
        spots = lax.broadcasted_iota(jnp.int32, (nodes, part), 1) + (gz * PARTS + b) * part
        pick_s[b] = jnp.where((ids == near) & (spots < live), 1.0, 0.0).astype(BF16)

    for copy in w2r_in:
        copy.wait()
    gain_own = cols[0, own(gz), :]
    first = latent // 2

    lines = share * 2 * sub

    def layers(t_in, hid_out, hid_in, spot, base):
        pieces = []
        for r in range(2):
            rows = slice(r * first, (r + 1) * first)
            h = dot(w1p[rows, :], xc[t_in])
            pieces.append(dot(w2r_v[rows, :], hid_in[...]))
            hid_out[rows, :] = half_silu(h)
            if r == 0:
                shift = jnp.mean(pieces[0], axis=0, keepdims=True)
                d = pieces[0] - shift
                d_own = d[:share]
                squares = jnp.sum(d * d, axis=0, keepdims=True)
            else:
                d = pieces[1] - shift
                lean = jnp.sum(d, axis=0, keepdims=True) * (1.0 / latent)
                squares = squares + jnp.sum(d * d, axis=0, keepdims=True)
        spread = squares * (1.0 / latent) - lean * lean
        out = (d_own - lean) * lax.rsqrt(spread + EPS) * wide(gain_own, sub)
        for l in range(sub):
            outf[pl.ds(base + spot * sub + l, share, stride=2 * sub), :] = out[:, l * lon_cols : (l + 1) * lon_cols]

    def settle(u):
        base = pl.multiple_of(lax.rem(u, 2) * lines, lines)
        out_blocks[u] = outf[pl.ds(base, lines), :].reshape(share, 2 * sub, lon_cols).astype(BF16)

    def pair(u, carry):
        settle(jnp.maximum(u - 1, 0))
        base = lax.rem(u, 2) * lines
        layers(2 * u + 1, hid_b, hid_a, 0, base)
        layers(jnp.minimum(2 * u + 2, tiles - 1), hid_a, hid_b, 1, base)
        return carry

    def embed(start, stop):
        lax.fori_loop(start, stop, pair, 0)

    hid_a[...] = half_silu(dot(w1p[...], xc[0]))
    outf[...] = jnp.zeros_like(outf)
    stops = FILL + (tiles // 2,)
    embed(0, stops[0])
    for copy in side_moves:
        copy.wait()
    corner_moves = [
        send(west.at[blocks - 1], corner.at[0], {"gx": down}),
        send(east.at[blocks - 1], corner.at[1], {"gx": down}),
        send(west.at[0], corner.at[2], {"gx": up}),
        send(east.at[0], corner.at[3], {"gx": up}),
    ]

    for copy in row_moves:
        copy.wait()
    half = KPAD * HALO
    xf[pl.ds(channels * HALO, (KPAD - channels) * HALO), :] = pad_values[0 : (KPAD - channels) * HALO] * 0.0 + jnp.where(
        lax.broadcasted_iota(jnp.int32, ((KPAD - channels) * HALO, 128), 0) < 3 * HALO, 1.0, 0.0
    ).astype(F32)
    for n, ref in enumerate((north, south)):
        xf[pl.ds(0, channels * HALO), :] = ref[...].astype(F32).reshape(channels * HALO, lon_cols)
        for l in range(HALO):
            xh[n, :, l * lon_cols : (l + 1) * lon_cols] = xf[pl.ds(l, KPAD, stride=HALO), :].astype(BF16)
    acc = gath[...]
    wing = HALO * lon_cols
    acc = acc + dot(xh[0], onehot(base_n, wing)) + dot(xh[1], onehot(base_s, wing))
    for i in range(blocks):
        acc = acc + dot(west[i], onehot(base_w + i * 128, 128)) + dot(east[i], onehot(base_e + i * 128, 128))
    gath[...] = acc
    embed(stops[0], stops[1])
    for copy in corner_moves:
        copy.wait()
    acc = gath[...]
    for i in range(4):
        acc = acc + dot(corner[i], onehot(base_c + i * 128, 128))
    picked = acc.astype(BF16)

    w2_in.wait()
    c, inv = centred(dot(w2_v[...], half_silu(dot(w1p[...], picked))))
    sender_latent = (c * inv * wide(cols[0], mine // 128)).astype(BF16)
    ew1_in.wait()
    for b in range(PARTS):
        pre_s[b] = dot(ew1_v[:, latent : 2 * latent], sender_latent[:, b * part : (b + 1) * part]) + wide(
            cols[1], part // 128
        )

    def edge_net(b):
        edge_in[b].wait()
        for copy in edge_moves[b]:
            copy.wait()
        pre = pre_s[b] + dot(ew1_v[:, :latent], edges[b])
        c, inv = centred(dot(ew2_v[...], half_silu(pre * 0.5)))
        part_sum = dot_nt((c * inv).astype(BF16), pick_s[b])
        tot[...] = part_sum if b == 0 else tot[...] + part_sum

    mesh_in.wait()
    for copy in mesh_moves:
        copy.wait()
    for b in range(PARTS):
        mesh_cols = dot(mesh_full[...], pick_s[b]).astype(BF16)
        pre_s[b] += dot(ew1_v[:, 2 * latent :], mesh_cols)
    ew2_in.wait()
    for b in range(PARTS):
        embed(stops[b + 1], stops[b + 2])
        edge_net(b)
    half = share // 2

    def sums(p, k):
        return tot[pl.ds(pl.multiple_of(p * share + k * half, 64), half), :]

    for k in range(2):
        tb[k] = sums(across, k).astype(BF16)
    tb[2] = sums(after, 1).astype(BF16)
    tb[3] = sums(before, 0).astype(BF16)
    relays = [send(tb.at[0], tr.at[0], {"gz": after}), send(tb.at[1], tr.at[1], {"gz": before})]
    sum_moves = [send(tb.at[2], tr.at[2], {"gz": after}), send(tb.at[3], tr.at[3], {"gz": before})]

    node_ids = lax.broadcasted_iota(jnp.int32, (nodes, slots), 0)
    slot_ids = lax.broadcasted_iota(jnp.int32, (nodes, slots), 1)
    pick = jnp.where((node_ids == recv_ref[...] - tile * nodes) & (slot_ids < live), 1.0, 0.0).astype(BF16)
    eown_in.wait()
    edge_sum = dot_nt(e_own[...], pick)
    degree = dot_nt(jnp.ones((8, slots), BF16), pick)[0:1, :]
    scale = 1.0 / jnp.maximum(degree, 1.0)
    gain_m = wide(cols[2, own(gz), :], nodes // 128)
    known = edge_sum + wide(cols[3, own(gz), :], nodes // 128) * degree
    mown_in.wait()
    for copy in relays:
        copy.wait()
    tb[4] = (sums(after, 0) + tr[0].astype(F32)).astype(BF16)
    tb[5] = (sums(before, 1) + tr[1].astype(F32)).astype(BF16)
    sum_moves += [send(tb.at[4], tr.at[4], {"gz": after}), send(tb.at[5], tr.at[5], {"gz": before})]
    embed(stops[PARTS + 1], stops[PARTS + 2])
    settle(tiles // 2 - 1)
    for copy in sum_moves:
        copy.wait()
    total = tot[own(gz), :] + jnp.concatenate(
        [tr[4].astype(F32) + tr[3].astype(F32), tr[2].astype(F32) + tr[5].astype(F32)], axis=0
    )
    out_mesh[...] = (mesh_own[...].astype(F32) + (known + gain_m * total) * scale).astype(BF16)


def deliver(mesh_ref, blocks_ref, out_mesh, out_grid, leave):
    count, _, rows, _ = blocks_ref.shape
    outs = [
        pltpu.make_async_copy(blocks_ref.at[u], out_grid.at[:, pl.ds(u * rows, rows), :], leave.at[u])
        for u in range(count)
    ]
    outs.append(pltpu.make_async_copy(mesh_ref, out_mesh, leave.at[count]))
    for copy in outs:
        copy.start()
    for copy in outs:
        copy.wait()


def on_device(
    sizes, grid_inputs, embed_w1, embed_b1, embed_w2, embed_gain, edge_w1, edge_b1, edge_w2,
    message_gain, message_bias, mesh_latent, edge_latent, senders, receivers, edge_counts,
):
    channels, lat_rows, lon_cols = grid_inputs.shape
    latent = embed_w2.shape[0]
    share, nodes, slots = mesh_latent.shape[0], mesh_latent.shape[3], edge_latent.shape[3]
    gz_n = sizes[2]
    mine = slots // gz_n
    blocks = lat_rows // ROWS
    tiles = lat_rows * lon_cols // TILE
    per = blocks and tiles // blocks
    anyspace = pl.BlockSpec(memory_space=pl.ANY)
    vmem = pl.BlockSpec(memory_space=pltpu.VMEM)
    smem = pl.BlockSpec(memory_space=pltpu.SMEM)
    V = pltpu.VMEM
    n_local = blocks + 1 + gz_n + 6 + PARTS + 7
    n_wire = PARTS * (gz_n - 1) + 20
    pairs, out_rows = tiles // 2, 2 * TILE // lon_cols
    mesh_out, grid_blocks = pl.pallas_call(
        functools.partial(kernel, sizes),
        out_shape=(
            pltpu.VMEM((share, nodes), BF16),
            pltpu.VMEM((pairs, share, out_rows, lon_cols), BF16),
        ),
        in_specs=[anyspace] * 14 + [smem],
        out_specs=(vmem, vmem),
        scratch_shapes=[
            V((blocks, channels, ROWS, lon_cols), BF16),
            V((channels, latent), BF16),
            V((latent, latent), BF16),
            V((latent, latent), BF16),
            V((latent, 3 * latent), BF16),
            V((latent, latent), BF16),
            V((share, slots), BF16),
            V((share, nodes), BF16),
            V((PARTS, latent, mine // PARTS), BF16),
            V((latent, nodes), BF16),
            V((channels, HALO, lon_cols), BF16),
            V((channels, HALO, lon_cols), BF16),
            V((blocks, KPAD, 128), BF16),
            V((blocks, KPAD, 128), BF16),
            V((4, KPAD, 128), BF16),
            V((KPAD * ROWS, lon_cols), F32),
            V((tiles, KPAD, TILE), BF16),
            V((2, KPAD, HALO * lon_cols), BF16),
            V((256, latent), F32),
            V((latent, KPAD), BF16),
            V((4, latent, 128), F32),
            V((per, TILE, 256), BF16),
            V((2, blocks, KPAD, 128), BF16),
            V((KPAD, mine), F32),
            V((2 * share * out_rows, lon_cols), F32),
            V((latent, nodes), F32),
            V((6, share // 2, nodes), BF16),
            V((6, share // 2, nodes), BF16),
            V((latent, TILE), BF16),
            V((latent, TILE), BF16),
            V((PARTS, latent, mine // PARTS), F32),
            V((PARTS, nodes, mine // PARTS), BF16),
            V((5, 1, latent), F32),
            V((1, slots), jnp.int32),
            V((1, slots), jnp.int32),
            pltpu.SemaphoreType.DMA((n_local,)),
            pltpu.SemaphoreType.DMA((n_wire,)),
            pltpu.SemaphoreType.DMA((n_wire,)),
        ],
        compiler_params=pltpu.CompilerParams(
            collective_id=0, has_side_effects=True, vmem_limit_bytes=56 * 1024 * 1024
        ),
    )(
        grid_inputs, embed_w1.T, embed_w2, edge_w1, edge_w2,
        embed_b1.reshape(1, latent), embed_gain.reshape(1, latent), edge_b1.reshape(1, latent),
        message_gain.reshape(1, latent), message_bias.reshape(1, latent),
        mesh_latent.reshape(share, nodes), edge_latent.reshape(share, slots),
        senders.reshape(1, slots), receivers.reshape(1, slots), edge_counts,
    )
    mesh_out, grid_out = pl.pallas_call(
        deliver,
        out_shape=(
            jax.ShapeDtypeStruct((share, nodes), BF16),
            jax.ShapeDtypeStruct((share, lat_rows, lon_cols), BF16),
        ),
        in_specs=[vmem, vmem],
        out_specs=(anyspace, anyspace),
        scratch_shapes=[pltpu.SemaphoreType.DMA((pairs + 1,))],
    )(
        pltpu.with_memory_space_constraint(mesh_out, pltpu.VMEM),
        pltpu.with_memory_space_constraint(grid_blocks, pltpu.VMEM),
    )
    return mesh_out.reshape(share, 1, 1, nodes), grid_out


def solution(mesh):
    sizes = (mesh.shape["gx"], mesh.shape["gy"], mesh.shape["gz"])
    return jax.shard_map(
        functools.partial(on_device, sizes),
        mesh=mesh,
        in_specs=(
            P(None, "gx", "gy"), P(), P(), P(), P(), P(), P(), P(), P(), P(),
            P("gz", "gx", "gy", None), P("gz", "gx", "gy", None),
            P("gx", "gy", None), P("gx", "gy", None), P("gx", "gy"),
        ),
        out_specs=(P("gz", "gx", "gy", None), P("gz", "gx", "gy")),
        check_vma=False,
    )
```

```python
import functools

import jax
import jax.numpy as jnp
from jax import lax
from jax.experimental import pallas as pl
from jax.experimental.pallas import tpu as pltpu
from jax.sharding import PartitionSpec as P

HALO = 8
EPS = 1e-05
FILL = (4, 6, 6, 6)
F32 = jnp.float32
BF16 = jnp.bfloat16
TILE = 512
PARTS = 2
ROWS = 16
KPAD = 192


def dot(a, b):
    return jnp.dot(a, b, preferred_element_type=F32)


def dot_nt(a, b):
    return lax.dot_general(a, b, (((1,), (1,)), ((), ())), preferred_element_type=F32)


def half_silu(h):
    return (h + h * jnp.tanh(h)).astype(BF16)


def centred(values):
    average = jnp.mean(values, axis=0, keepdims=True)
    c = values - average
    spread = jnp.mean(c * c, axis=0, keepdims=True)
    return c, lax.rsqrt(spread + EPS)


def wide(column, times):
    return jnp.concatenate([column] * times, axis=1)


def kernel(
    sizes,
    x_hbm, w1t_hbm, w2_hbm, ew1_hbm, ew2_hbm,
    b1_hbm, gain_hbm, eb1_hbm, mgain_hbm, mbias_hbm,
    mesh_hbm, edge_hbm, send_hbm, recv_hbm, count_ref,
    out_mesh, out_blocks,
    x_v, w1t_v, w2_v, w2r_v, ew1_v, ew2_v, e_own, mesh_own, edges, mesh_full,
    north, south, west, east, corner,
    xf, xc, xh, w1f, w1p, cols, sel, strip, gath, outf, tot, tb, tr,
    hid_a, hid_b, pre_s, pick_s,
    vecs, send_ref, recv_ref,
    local, wsend, wrecv,
):
    gx_n, gy_n, gz_n = sizes
    channels, lat_rows, lon_cols = x_hbm.shape
    latent = w2_v.shape[0]
    share = latent // gz_n
    slots = edge_hbm.shape[1]
    mine = slots // gz_n
    nodes = mesh_hbm.shape[1]
    blocks = lat_rows // ROWS
    gx, gy, gz = lax.axis_index("gx"), lax.axis_index("gy"), lax.axis_index("gz")
    up, down = lax.rem(gx + gx_n - 1, gx_n), lax.rem(gx + 1, gx_n)
    left, right = lax.rem(gy + gy_n - 1, gy_n), lax.rem(gy + 1, gy_n)
    peers = [lax.rem(gz + d, gz_n) for d in range(1, gz_n)]

    places = [{"gz": p} for p in peers]
    places += [{"gx": up}, {"gx": down}, {"gy": left}, {"gy": right}]
    y, z_lo = lax.rem(gy, 4), gy // 4
    lean_e = jnp.where(y == 3, jnp.where(z_lo == 0, gz_n - 1, 1), 0)
    lean_w = jnp.where(y == 0, jnp.where(z_lo == 0, gz_n - 1, 1), 0)
    east_place = {"gy": right, "gz": lax.rem(gz + lean_e, gz_n)}
    west_place = {"gy": left, "gz": lax.rem(gz + lean_w, gz_n)}
    places += [east_place, west_place]
    barrier = pltpu.get_barrier_semaphore()
    for place in places:
        pl.semaphore_signal(barrier, inc=1, device_id=place, device_id_type=pl.DeviceIdType.MESH)

    def own(index, size=share):
        return pl.ds(pl.multiple_of(index * size, 128), size)

    vec_hbm = (b1_hbm, gain_hbm, eb1_hbm, mgain_hbm, mbias_hbm)
    copies = []

    def bring(src, dst):
        copy = pltpu.make_async_copy(src, dst, local.at[len(copies)])
        copy.start()
        copies.append(copy)
        return copy

    w1_in = bring(w1t_hbm, w1t_v)
    vec_in = [bring(ref, vecs.at[k]) for k, ref in enumerate(vec_hbm)]
    x_in = [bring(x_hbm.at[:, pl.ds(i * ROWS, ROWS), :], x_v.at[i]) for i in range(blocks)]
    index_in = [bring(send_hbm, send_ref), bring(recv_hbm, recv_ref)]
    part = mine // PARTS
    pl.semaphore_wait(barrier, len(places))
    sent = []

    def send(src, dst, place):
        n = len(sent)
        copy = pltpu.make_async_remote_copy(
            src_ref=src, dst_ref=dst, send_sem=wsend.at[n], recv_sem=wrecv.at[n],
            device_id=place, device_id_type=pl.DeviceIdType.MESH,
        )
        copy.start()
        sent.append(copy)
        return copy

    after, across, before = peers
    mesh_moves = [send(mesh_hbm, mesh_full.at[own(gz), :], {"gz": p}) for p in (after, before)]

    def send_edges(b, p):
        return send(edge_hbm.at[:, own(p * PARTS + b, part)], edges.at[b, own(gz), :], {"gz": p})

    edge_moves = [[], []]
    row_moves = [
        send(x_hbm.at[:, pl.ds(0, HALO), :], south, {"gx": up}),
        send(x_hbm.at[:, pl.ds(lat_rows - HALO, HALO), :], north, {"gx": down}),
    ]
    w1_in.wait()
    for copy in vec_in:
        copy.wait()
    w1f[...] = jnp.zeros_like(w1f)
    w1f[0:channels, :] = w1t_v[...].astype(F32) * 0.5
    half_b = vecs[0] * 0.5
    for k in range(3):
        piece = half_b.astype(BF16).astype(F32)
        w1f[channels + k : channels + k + 1, :] = piece
        half_b = half_b - piece
    w1p[...] = jnp.transpose(w1f[...])[:, :KPAD].astype(BF16)
    for k in range(4):
        cols[k] = jnp.transpose(jnp.broadcast_to(vecs[k + 1], (128, latent)))
    pad_rows = lax.broadcasted_iota(jnp.int32, ((KPAD - channels) * ROWS, 128), 0)
    pad_values = jnp.where(pad_rows < 3 * ROWS, 1.0, 0.0).astype(F32)
    xf[pl.ds(channels * ROWS, (KPAD - channels) * ROWS), :] = pad_values

    sub = TILE // lon_cols
    for q in range(ROWS // sub):
        k = lax.broadcasted_iota(jnp.int32, (TILE, 256), 0)
        j = lax.broadcasted_iota(jnp.int32, (TILE, 256), 1)
        side, jj = j >> 7, j & 127
        want = ((jj >> 3) - q * sub) * lon_cols + side * (lon_cols - HALO) + (jj & 7)
        sel[q] = jnp.where(k == want, 1.0, 0.0).astype(BF16)

    per = ROWS // sub

    def relayout(i, carry):
        xf[pl.ds(0, channels * ROWS), :] = x_v[i].astype(F32).reshape(channels * ROWS, lon_cols)
        for l in range(ROWS):
            line = xf[pl.ds(l, KPAD, stride=ROWS), :].astype(BF16)
            xc[i * per + l // sub, :, (l % sub) * lon_cols : (l % sub + 1) * lon_cols] = line
        acc = dot(xc[i * per], sel[0])
        for q in range(1, per):
            acc = acc + dot(xc[i * per + q], sel[q])
        strip[0, i] = acc[:, :128].astype(BF16)
        strip[1, i] = acc[:, 128:].astype(BF16)
        return carry

    for copy in x_in:
        copy.wait()
    lax.fori_loop(0, blocks, relayout, 0)
    cut = blocks // 2
    side_moves = [
        send(strip.at[0, pl.ds(0, cut)], east.at[pl.ds(0, cut)], {"gy": left}),
        send(strip.at[1, pl.ds(0, cut)], west.at[pl.ds(0, cut)], {"gy": right}),
        send(strip.at[0, pl.ds(cut, cut)], east.at[pl.ds(cut, cut)], west_place),
        send(strip.at[1, pl.ds(cut, cut)], west.at[pl.ds(cut, cut)], east_place),
    ]
    edge_moves[0] += [send_edges(0, p) for p in (across, after, before)]
    w2r_in = [
        bring(w2_hbm.at[own(lax.rem(gz + j, gz_n)), :], w2r_v.at[pl.ds(j * share, share), :])
        for j in range(gz_n)
    ]
    w2_in = bring(w2_hbm, w2_v)
    edge_in = [
        bring(edge_hbm.at[:, own(gz * PARTS + b, part)], edges.at[b, own(gz), :]) for b in range(PARTS)
    ]
    mesh_in = bring(mesh_hbm, mesh_full.at[own(gz), :])
    mown_in = bring(mesh_hbm, mesh_own)
    eown_in = bring(edge_hbm, e_own)
    ew1_in = bring(ew1_hbm, ew1_v)
    ew2_in = bring(ew2_hbm, ew2_v)

    for copy in index_in:
        copy.wait()
    sender = send_ref[:, own(gz, mine)]
    lon_total = gy_n * lon_cols
    rl = sender // lon_total - gx * lat_rows + HALO
    cl = sender % lon_total - gy * lon_cols + HALO + lon_total
    cl = cl % lon_total
    cells = lat_rows * lon_cols
    base_n, base_s = cells, cells + HALO * lon_cols
    base_w = cells + 2 * HALO * lon_cols
    base_e = base_w + HALO * lat_rows
    base_c = base_e + HALO * lat_rows
    is_n, is_s = rl < HALO, rl >= lat_rows + HALO
    is_w, is_e = cl < HALO, cl >= lon_cols + HALO
    c_in = jnp.where(is_w, cl, cl - (lon_cols + HALO))
    middle = jnp.where(
        is_n, base_n + rl * lon_cols,
        jnp.where(is_s, base_s + (rl - lat_rows - HALO) * lon_cols, (rl - HALO) * lon_cols),
    ) + cl - HALO
    aside = jnp.where(is_w, base_w, base_e) + (rl - HALO) * HALO + c_in
    cornered = (
        base_c
        + jnp.where(is_n, 0, 2 * 128)
        + jnp.where(is_w, 0, 128)
        + jnp.where(is_n, (rl + ROWS - HALO) * HALO, (rl - lat_rows - HALO) * HALO)
        + c_in
    )
    place_of = jnp.where(is_w | is_e, jnp.where(is_n | is_s, cornered, aside), middle)

    def onehot(base, size):
        ids = lax.broadcasted_iota(jnp.int32, (size, mine), 0)
        return jnp.where(ids == place_of - base, 1.0, 0.0).astype(BF16)

    gath[...] = jnp.zeros_like(gath)

    def gather(t, carry):
        found = dot(xc[t * per], onehot(t * per * TILE, TILE))
        for q in range(1, per):
            found = found + dot(xc[t * per + q], onehot((t * per + q) * TILE, TILE))
        gath[...] += found
        return carry

    tiles = cells // TILE
    lax.fori_loop(0, blocks, gather, 0)

    for copy in mesh_moves:
        copy.wait()
    upper = mesh_full.at[pl.ds(pl.multiple_of(before * share, 128), share // 2), :]
    lower = mesh_full.at[pl.ds(pl.multiple_of(after * share + share // 2, 64), share // 2), :]
    mesh_moves = [send(upper, upper, {"gz": after}), send(lower, lower, {"gz": before})]
    edge_moves[1] = [send_edges(1, p) for p in (across, after, before)]

    live = count_ref[0, 0]
    tile = gx * gy_n + gy
    for b in range(PARTS):
        near = recv_ref[:, own(gz * PARTS + b, part)] - tile * nodes
        ids = lax.broadcasted_iota(jnp.int32, (nodes, part), 0)
        spots = lax.broadcasted_iota(jnp.int32, (nodes, part), 1) + (gz * PARTS + b) * part
        pick_s[b] = jnp.where((ids == near) & (spots < live), 1.0, 0.0).astype(BF16)

    for copy in w2r_in:
        copy.wait()
    gain_own = cols[0, own(gz), :]
    first = latent // 2

    lines = share * 2 * sub

    def layers(t_in, hid_out, hid_in, spot, base):
        pieces = []
        for r in range(2):
            rows = slice(r * first, (r + 1) * first)
            h = dot(w1p[rows, :], xc[t_in])
            pieces.append(dot(w2r_v[rows, :], hid_in[...]))
            hid_out[rows, :] = half_silu(h)
            if r == 0:
                shift = jnp.mean(pieces[0], axis=0, keepdims=True)
                d = pieces[0] - shift
                d_own = d[:share]
                squares = jnp.sum(d * d, axis=0, keepdims=True)
            else:
                d = pieces[1] - shift
                lean = jnp.sum(d, axis=0, keepdims=True) * (1.0 / latent)
                squares = squares + jnp.sum(d * d, axis=0, keepdims=True)
        spread = squares * (1.0 / latent) - lean * lean
        out = (d_own - lean) * lax.rsqrt(spread + EPS) * wide(gain_own, sub)
        for l in range(sub):
            outf[pl.ds(base + spot * sub + l, share, stride=2 * sub), :] = out[:, l * lon_cols : (l + 1) * lon_cols]

    def settle(u):
        base = pl.multiple_of(lax.rem(u, 2) * lines, lines)
        out_blocks[u] = outf[pl.ds(base, lines), :].reshape(share, 2 * sub, lon_cols).astype(BF16)

    def pair(u, carry):
        settle(jnp.maximum(u - 1, 0))
        base = lax.rem(u, 2) * lines
        layers(2 * u + 1, hid_b, hid_a, 0, base)
        layers(jnp.minimum(2 * u + 2, tiles - 1), hid_a, hid_b, 1, base)
        return carry

    def embed(start, stop):
        lax.fori_loop(start, stop, pair, 0)

    hid_a[...] = half_silu(dot(w1p[...], xc[0]))
    outf[...] = jnp.zeros_like(outf)
    stops = FILL + (tiles // 2,)
    embed(0, stops[0])
    for copy in side_moves:
        copy.wait()
    corner_moves = [
        send(west.at[blocks - 1], corner.at[0], {"gx": down}),
        send(east.at[blocks - 1], corner.at[1], {"gx": down}),
        send(west.at[0], corner.at[2], {"gx": up}),
        send(east.at[0], corner.at[3], {"gx": up}),
    ]

    for copy in row_moves:
        copy.wait()
    half = KPAD * HALO
    xf[pl.ds(channels * HALO, (KPAD - channels) * HALO), :] = pad_values[0 : (KPAD - channels) * HALO] * 0.0 + jnp.where(
        lax.broadcasted_iota(jnp.int32, ((KPAD - channels) * HALO, 128), 0) < 3 * HALO, 1.0, 0.0
    ).astype(F32)
    for n, ref in enumerate((north, south)):
        xf[pl.ds(0, channels * HALO), :] = ref[...].astype(F32).reshape(channels * HALO, lon_cols)
        for l in range(HALO):
            xh[n, :, l * lon_cols : (l + 1) * lon_cols] = xf[pl.ds(l, KPAD, stride=HALO), :].astype(BF16)
    acc = gath[...]
    wing = HALO * lon_cols
    acc = acc + dot(xh[0], onehot(base_n, wing)) + dot(xh[1], onehot(base_s, wing))
    for i in range(blocks):
        acc = acc + dot(west[i], onehot(base_w + i * 128, 128)) + dot(east[i], onehot(base_e + i * 128, 128))
    gath[...] = acc
    embed(stops[0], stops[1])
    for copy in corner_moves:
        copy.wait()
    acc = gath[...]
    for i in range(4):
        acc = acc + dot(corner[i], onehot(base_c + i * 128, 128))
    picked = acc.astype(BF16)

    w2_in.wait()
    c, inv = centred(dot(w2_v[...], half_silu(dot(w1p[...], picked))))
    sender_latent = (c * inv * wide(cols[0], mine // 128)).astype(BF16)
    ew1_in.wait()
    for b in range(PARTS):
        pre_s[b] = dot(ew1_v[:, latent : 2 * latent], sender_latent[:, b * part : (b + 1) * part]) + wide(
            cols[1], part // 128
        )

    def edge_net(b):
        edge_in[b].wait()
        for copy in edge_moves[b]:
            copy.wait()
        pre = pre_s[b] + dot(ew1_v[:, :latent], edges[b])
        c, inv = centred(dot(ew2_v[...], half_silu(pre * 0.5)))
        part_sum = dot_nt((c * inv).astype(BF16), pick_s[b])
        tot[...] = part_sum if b == 0 else tot[...] + part_sum

    mesh_in.wait()
    for copy in mesh_moves:
        copy.wait()
    for b in range(PARTS):
        mesh_cols = dot(mesh_full[...], pick_s[b]).astype(BF16)
        pre_s[b] += dot(ew1_v[:, 2 * latent :], mesh_cols)
    ew2_in.wait()
    for b in range(PARTS):
        embed(stops[b + 1], stops[b + 2])
        edge_net(b)
    half = share // 2

    def sums(p, k):
        return tot[pl.ds(pl.multiple_of(p * share + k * half, 64), half), :]

    for k in range(2):
        tb[k] = sums(across, k).astype(BF16)
    tb[2] = sums(after, 1).astype(BF16)
    tb[3] = sums(before, 0).astype(BF16)
    relays = [send(tb.at[0], tr.at[0], {"gz": after}), send(tb.at[1], tr.at[1], {"gz": before})]
    sum_moves = [send(tb.at[2], tr.at[2], {"gz": after}), send(tb.at[3], tr.at[3], {"gz": before})]

    node_ids = lax.broadcasted_iota(jnp.int32, (nodes, slots), 0)
    slot_ids = lax.broadcasted_iota(jnp.int32, (nodes, slots), 1)
    pick = jnp.where((node_ids == recv_ref[...] - tile * nodes) & (slot_ids < live), 1.0, 0.0).astype(BF16)
    eown_in.wait()
    edge_sum = dot_nt(e_own[...], pick)
    degree = dot_nt(jnp.ones((8, slots), BF16), pick)[0:1, :]
    scale = 1.0 / jnp.maximum(degree, 1.0)
    gain_m = wide(cols[2, own(gz), :], nodes // 128)
    known = edge_sum + wide(cols[3, own(gz), :], nodes // 128) * degree
    mown_in.wait()
    spare = stops[PARTS + 1] + 1
    embed(stops[PARTS + 1], spare)
    for copy in relays:
        copy.wait()
    tb[4] = (sums(after, 0) + tr[0].astype(F32)).astype(BF16)
    tb[5] = (sums(before, 1) + tr[1].astype(F32)).astype(BF16)
    sum_moves += [send(tb.at[4], tr.at[4], {"gz": after}), send(tb.at[5], tr.at[5], {"gz": before})]
    embed(spare, stops[PARTS + 2])
    settle(tiles // 2 - 1)
    for copy in sum_moves:
        copy.wait()
    total = tot[own(gz), :] + jnp.concatenate(
        [tr[4].astype(F32) + tr[3].astype(F32), tr[2].astype(F32) + tr[5].astype(F32)], axis=0
    )
    out_mesh[...] = (mesh_own[...].astype(F32) + (known + gain_m * total) * scale).astype(BF16)


def deliver(mesh_ref, blocks_ref, out_mesh, out_grid, leave):
    count, _, rows, _ = blocks_ref.shape
    outs = [
        pltpu.make_async_copy(blocks_ref.at[u], out_grid.at[:, pl.ds(u * rows, rows), :], leave.at[u])
        for u in range(count)
    ]
    outs.append(pltpu.make_async_copy(mesh_ref, out_mesh, leave.at[count]))
    for copy in outs:
        copy.start()
    for copy in outs:
        copy.wait()


def on_device(
    sizes, grid_inputs, embed_w1, embed_b1, embed_w2, embed_gain, edge_w1, edge_b1, edge_w2,
    message_gain, message_bias, mesh_latent, edge_latent, senders, receivers, edge_counts,
):
    channels, lat_rows, lon_cols = grid_inputs.shape
    latent = embed_w2.shape[0]
    share, nodes, slots = mesh_latent.shape[0], mesh_latent.shape[3], edge_latent.shape[3]
    gz_n = sizes[2]
    mine = slots // gz_n
    blocks = lat_rows // ROWS
    tiles = lat_rows * lon_cols // TILE
    per = blocks and tiles // blocks
    anyspace = pl.BlockSpec(memory_space=pl.ANY)
    vmem = pl.BlockSpec(memory_space=pltpu.VMEM)
    smem = pl.BlockSpec(memory_space=pltpu.SMEM)
    V = pltpu.VMEM
    n_local = blocks + 1 + gz_n + 6 + PARTS + 7
    n_wire = PARTS * (gz_n - 1) + 20
    pairs, out_rows = tiles // 2, 2 * TILE // lon_cols
    mesh_out, grid_blocks = pl.pallas_call(
        functools.partial(kernel, sizes),
        out_shape=(
            pltpu.VMEM((share, nodes), BF16),
            pltpu.VMEM((pairs, share, out_rows, lon_cols), BF16),
        ),
        in_specs=[anyspace] * 14 + [smem],
        out_specs=(vmem, vmem),
        scratch_shapes=[
            V((blocks, channels, ROWS, lon_cols), BF16),
            V((channels, latent), BF16),
            V((latent, latent), BF16),
            V((latent, latent), BF16),
            V((latent, 3 * latent), BF16),
            V((latent, latent), BF16),
            V((share, slots), BF16),
            V((share, nodes), BF16),
            V((PARTS, latent, mine // PARTS), BF16),
            V((latent, nodes), BF16),
            V((channels, HALO, lon_cols), BF16),
            V((channels, HALO, lon_cols), BF16),
            V((blocks, KPAD, 128), BF16),
            V((blocks, KPAD, 128), BF16),
            V((4, KPAD, 128), BF16),
            V((KPAD * ROWS, lon_cols), F32),
            V((tiles, KPAD, TILE), BF16),
            V((2, KPAD, HALO * lon_cols), BF16),
            V((256, latent), F32),
            V((latent, KPAD), BF16),
            V((4, latent, 128), F32),
            V((per, TILE, 256), BF16),
            V((2, blocks, KPAD, 128), BF16),
            V((KPAD, mine), F32),
            V((2 * share * out_rows, lon_cols), F32),
            V((latent, nodes), F32),
            V((6, share // 2, nodes), BF16),
            V((6, share // 2, nodes), BF16),
            V((latent, TILE), BF16),
            V((latent, TILE), BF16),
            V((PARTS, latent, mine // PARTS), F32),
            V((PARTS, nodes, mine // PARTS), BF16),
            V((5, 1, latent), F32),
            V((1, slots), jnp.int32),
            V((1, slots), jnp.int32),
            pltpu.SemaphoreType.DMA((n_local,)),
            pltpu.SemaphoreType.DMA((n_wire,)),
            pltpu.SemaphoreType.DMA((n_wire,)),
        ],
        compiler_params=pltpu.CompilerParams(
            collective_id=0, has_side_effects=True, vmem_limit_bytes=56 * 1024 * 1024
        ),
    )(
        grid_inputs, embed_w1.T, embed_w2, edge_w1, edge_w2,
        embed_b1.reshape(1, latent), embed_gain.reshape(1, latent), edge_b1.reshape(1, latent),
        message_gain.reshape(1, latent), message_bias.reshape(1, latent),
        mesh_latent.reshape(share, nodes), edge_latent.reshape(share, slots),
        senders.reshape(1, slots), receivers.reshape(1, slots), edge_counts,
    )
    mesh_out, grid_out = pl.pallas_call(
        deliver,
        out_shape=(
            jax.ShapeDtypeStruct((share, nodes), BF16),
            jax.ShapeDtypeStruct((share, lat_rows, lon_cols), BF16),
        ),
        in_specs=[vmem, vmem],
        out_specs=(anyspace, anyspace),
        scratch_shapes=[pltpu.SemaphoreType.DMA((pairs + 1,))],
    )(
        pltpu.with_memory_space_constraint(mesh_out, pltpu.VMEM),
        pltpu.with_memory_space_constraint(grid_blocks, pltpu.VMEM),
    )
    return mesh_out.reshape(share, 1, 1, nodes), grid_out


def solution(mesh):
    sizes = (mesh.shape["gx"], mesh.shape["gy"], mesh.shape["gz"])
    return jax.shard_map(
        functools.partial(on_device, sizes),
        mesh=mesh,
        in_specs=(
            P(None, "gx", "gy"), P(), P(), P(), P(), P(), P(), P(), P(), P(),
            P("gz", "gx", "gy", None), P("gz", "gx", "gy", None),
            P("gx", "gy", None), P("gx", "gy", None), P("gx", "gy"),
        ),
        out_specs=(P("gz", "gx", "gy", None), P("gz", "gx", "gy")),
        check_vma=False,
    )
```

```python
import functools

import jax
import jax.numpy as jnp
from jax import lax
from jax.experimental import pallas as pl
from jax.experimental.pallas import tpu as pltpu
from jax.sharding import PartitionSpec as P

HALO = 8
EPS = 1e-05
FILL = (4, 6, 6, 6)
F32 = jnp.float32
BF16 = jnp.bfloat16
TILE = 512
PARTS = 2
ROWS = 16
KPAD = 192


def dot(a, b):
    return jnp.dot(a, b, preferred_element_type=F32)


def dot_nt(a, b):
    return lax.dot_general(a, b, (((1,), (1,)), ((), ())), preferred_element_type=F32)


def half_silu(h):
    return (h + h * jnp.tanh(h)).astype(BF16)


def centred(values):
    average = jnp.mean(values, axis=0, keepdims=True)
    c = values - average
    spread = jnp.mean(c * c, axis=0, keepdims=True)
    return c, lax.rsqrt(spread + EPS)


def wide(column, times):
    return jnp.concatenate([column] * times, axis=1)


def kernel(
    sizes,
    x_hbm, w1t_hbm, w2_hbm, ew1_hbm, ew2_hbm,
    b1_hbm, gain_hbm, eb1_hbm, mgain_hbm, mbias_hbm,
    mesh_hbm, edge_hbm, send_hbm, recv_hbm, count_ref,
    out_mesh, out_blocks,
    x_v, w1t_v, w2_v, w2r_v, ew1_v, ew2_v, e_own, mesh_own, edges, mesh_full,
    north, south, west, east, corner,
    xf, xc, xh, w1f, w1p, cols, sel, strip, gath, outf, tot, tb, tr,
    hid_a, hid_b, pre_s, pick_s,
    vecs, send_ref, recv_ref,
    local, wsend, wrecv,
):
    gx_n, gy_n, gz_n = sizes
    channels, lat_rows, lon_cols = x_hbm.shape
    latent = w2_v.shape[0]
    share = latent // gz_n
    slots = edge_hbm.shape[1]
    mine = slots // gz_n
    nodes = mesh_hbm.shape[1]
    blocks = lat_rows // ROWS
    gx, gy, gz = lax.axis_index("gx"), lax.axis_index("gy"), lax.axis_index("gz")
    up, down = lax.rem(gx + gx_n - 1, gx_n), lax.rem(gx + 1, gx_n)
    left, right = lax.rem(gy + gy_n - 1, gy_n), lax.rem(gy + 1, gy_n)
    peers = [lax.rem(gz + d, gz_n) for d in range(1, gz_n)]

    places = [{"gz": p} for p in peers]
    places += [{"gx": up}, {"gx": down}, {"gy": left}, {"gy": right}]
    y, z_lo = lax.rem(gy, 4), gy // 4
    lean_e = jnp.where(y == 3, jnp.where(z_lo == 0, gz_n - 1, 1), 0)
    lean_w = jnp.where(y == 0, jnp.where(z_lo == 0, gz_n - 1, 1), 0)
    east_place = {"gy": right, "gz": lax.rem(gz + lean_e, gz_n)}
    west_place = {"gy": left, "gz": lax.rem(gz + lean_w, gz_n)}
    places += [east_place, west_place]
    barrier = pltpu.get_barrier_semaphore()
    for place in places:
        pl.semaphore_signal(barrier, inc=1, device_id=place, device_id_type=pl.DeviceIdType.MESH)

    def own(index, size=share):
        return pl.ds(pl.multiple_of(index * size, 128), size)

    vec_hbm = (b1_hbm, gain_hbm, eb1_hbm, mgain_hbm, mbias_hbm)
    copies = []

    def bring(src, dst):
        copy = pltpu.make_async_copy(src, dst, local.at[len(copies)])
        copy.start()
        copies.append(copy)
        return copy

    w1_in = bring(w1t_hbm, w1t_v)
    vec_in = [bring(ref, vecs.at[k]) for k, ref in enumerate(vec_hbm)]
    x_in = [bring(x_hbm.at[:, pl.ds(i * ROWS, ROWS), :], x_v.at[i]) for i in range(blocks)]
    index_in = [bring(send_hbm, send_ref), bring(recv_hbm, recv_ref)]
    part = mine // PARTS
    pl.semaphore_wait(barrier, len(places))
    sent = []

    def send(src, dst, place):
        n = len(sent)
        copy = pltpu.make_async_remote_copy(
            src_ref=src, dst_ref=dst, send_sem=wsend.at[n], recv_sem=wrecv.at[n],
            device_id=place, device_id_type=pl.DeviceIdType.MESH,
        )
        copy.start()
        sent.append(copy)
        return copy

    after, across, before = peers
    mesh_moves = [send(mesh_hbm, mesh_full.at[own(gz), :], {"gz": p}) for p in (after, before)]

    def send_edges(b, p):
        return send(edge_hbm.at[:, own(p * PARTS + b, part)], edges.at[b, own(gz), :], {"gz": p})

    edge_moves = [[], []]
    row_moves = [
        send(x_hbm.at[:, pl.ds(0, HALO), :], south, {"gx": up}),
        send(x_hbm.at[:, pl.ds(lat_rows - HALO, HALO), :], north, {"gx": down}),
    ]
    w1_in.wait()
    for copy in vec_in:
        copy.wait()
    w1f[...] = jnp.zeros_like(w1f)
    w1f[0:channels, :] = w1t_v[...].astype(F32) * 0.5
    half_b = vecs[0] * 0.5
    for k in range(3):
        piece = half_b.astype(BF16).astype(F32)
        w1f[channels + k : channels + k + 1, :] = piece
        half_b = half_b - piece
    w1p[...] = jnp.transpose(w1f[...])[:, :KPAD].astype(BF16)
    for k in range(4):
        cols[k] = jnp.transpose(jnp.broadcast_to(vecs[k + 1], (128, latent)))
    pad_rows = lax.broadcasted_iota(jnp.int32, ((KPAD - channels) * ROWS, 128), 0)
    pad_values = jnp.where(pad_rows < 3 * ROWS, 1.0, 0.0).astype(F32)
    xf[pl.ds(channels * ROWS, (KPAD - channels) * ROWS), :] = pad_values

    sub = TILE // lon_cols
    for q in range(ROWS // sub):
        k = lax.broadcasted_iota(jnp.int32, (TILE, 256), 0)
        j = lax.broadcasted_iota(jnp.int32, (TILE, 256), 1)
        side, jj = j >> 7, j & 127
        want = ((jj >> 3) - q * sub) * lon_cols + side * (lon_cols - HALO) + (jj & 7)
        sel[q] = jnp.where(k == want, 1.0, 0.0).astype(BF16)

    per = ROWS // sub

    def relayout(i, carry):
        xf[pl.ds(0, channels * ROWS), :] = x_v[i].astype(F32).reshape(channels * ROWS, lon_cols)
        for l in range(ROWS):
            line = xf[pl.ds(l, KPAD, stride=ROWS), :].astype(BF16)
            xc[i * per + l // sub, :, (l % sub) * lon_cols : (l % sub + 1) * lon_cols] = line
        acc = dot(xc[i * per], sel[0])
        for q in range(1, per):
            acc = acc + dot(xc[i * per + q], sel[q])
        strip[0, i] = acc[:, :128].astype(BF16)
        strip[1, i] = acc[:, 128:].astype(BF16)
        return carry

    for copy in x_in:
        copy.wait()
    lax.fori_loop(0, blocks, relayout, 0)
    cut = blocks // 2
    side_moves = [
        send(strip.at[0, pl.ds(0, cut)], east.at[pl.ds(0, cut)], {"gy": left}),
        send(strip.at[1, pl.ds(0, cut)], west.at[pl.ds(0, cut)], {"gy": right}),
        send(strip.at[0, pl.ds(cut, cut)], east.at[pl.ds(cut, cut)], west_place),
        send(strip.at[1, pl.ds(cut, cut)], west.at[pl.ds(cut, cut)], east_place),
    ]
    edge_moves[0] += [send_edges(0, p) for p in (across, after, before)]
    w2r_in = [
        bring(w2_hbm.at[own(lax.rem(gz + j, gz_n)), :], w2r_v.at[pl.ds(j * share, share), :])
        for j in range(gz_n)
    ]
    w2_in = bring(w2_hbm, w2_v)
    edge_in = [
        bring(edge_hbm.at[:, own(gz * PARTS + b, part)], edges.at[b, own(gz), :]) for b in range(PARTS)
    ]
    mesh_in = bring(mesh_hbm, mesh_full.at[own(gz), :])
    mown_in = bring(mesh_hbm, mesh_own)
    eown_in = bring(edge_hbm, e_own)
    ew1_in = bring(ew1_hbm, ew1_v)
    ew2_in = bring(ew2_hbm, ew2_v)

    for copy in index_in:
        copy.wait()
    sender = send_ref[:, own(gz, mine)]
    lon_total = gy_n * lon_cols
    rl = sender // lon_total - gx * lat_rows + HALO
    cl = sender % lon_total - gy * lon_cols + HALO + lon_total
    cl = cl % lon_total
    cells = lat_rows * lon_cols
    base_n, base_s = cells, cells + HALO * lon_cols
    base_w = cells + 2 * HALO * lon_cols
    base_e = base_w + HALO * lat_rows
    base_c = base_e + HALO * lat_rows
    is_n, is_s = rl < HALO, rl >= lat_rows + HALO
    is_w, is_e = cl < HALO, cl >= lon_cols + HALO
    c_in = jnp.where(is_w, cl, cl - (lon_cols + HALO))
    middle = jnp.where(
        is_n, base_n + rl * lon_cols,
        jnp.where(is_s, base_s + (rl - lat_rows - HALO) * lon_cols, (rl - HALO) * lon_cols),
    ) + cl - HALO
    aside = jnp.where(is_w, base_w, base_e) + (rl - HALO) * HALO + c_in
    cornered = (
        base_c
        + jnp.where(is_n, 0, 2 * 128)
        + jnp.where(is_w, 0, 128)
        + jnp.where(is_n, (rl + ROWS - HALO) * HALO, (rl - lat_rows - HALO) * HALO)
        + c_in
    )
    place_of = jnp.where(is_w | is_e, jnp.where(is_n | is_s, cornered, aside), middle)

    def onehot(base, size):
        ids = lax.broadcasted_iota(jnp.int32, (size, mine), 0)
        return jnp.where(ids == place_of - base, 1.0, 0.0).astype(BF16)

    gath[...] = jnp.zeros_like(gath)

    def gather(t, carry):
        found = dot(xc[t * per], onehot(t * per * TILE, TILE))
        for q in range(1, per):
            found = found + dot(xc[t * per + q], onehot((t * per + q) * TILE, TILE))
        gath[...] += found
        return carry

    tiles = cells // TILE
    lax.fori_loop(0, blocks, gather, 0)

    for copy in mesh_moves:
        copy.wait()
    upper = mesh_full.at[pl.ds(pl.multiple_of(before * share, 128), share // 2), :]
    lower = mesh_full.at[pl.ds(pl.multiple_of(after * share + share // 2, 64), share // 2), :]
    mesh_moves = [send(upper, upper, {"gz": after}), send(lower, lower, {"gz": before})]
    edge_moves[1] = [send_edges(1, p) for p in (across, after, before)]

    live = count_ref[0, 0]
    tile = gx * gy_n + gy
    for b in range(PARTS):
        near = recv_ref[:, own(gz * PARTS + b, part)] - tile * nodes
        ids = lax.broadcasted_iota(jnp.int32, (nodes, part), 0)
        spots = lax.broadcasted_iota(jnp.int32, (nodes, part), 1) + (gz * PARTS + b) * part
        pick_s[b] = jnp.where((ids == near) & (spots < live), 1.0, 0.0).astype(BF16)

    for copy in w2r_in:
        copy.wait()
    gain_own = cols[0, own(gz), :]
    first = latent // 2

    lines = share * 2 * sub

    def layers(t_in, hid_out, hid_in, spot, base):
        pieces = []
        for r in range(2):
            rows = slice(r * first, (r + 1) * first)
            h = dot(w1p[rows, :], xc[t_in])
            pieces.append(dot(w2r_v[rows, :], hid_in[...]))
            hid_out[rows, :] = half_silu(h)
            if r == 0:
                shift = jnp.mean(pieces[0], axis=0, keepdims=True)
                d = pieces[0] - shift
                d_own = d[:share]
                squares = jnp.sum(d * d, axis=0, keepdims=True)
            else:
                d = pieces[1] - shift
                lean = jnp.sum(d, axis=0, keepdims=True) * (1.0 / latent)
                squares = squares + jnp.sum(d * d, axis=0, keepdims=True)
        spread = squares * (1.0 / latent) - lean * lean
        out = (d_own - lean) * lax.rsqrt(spread + EPS) * wide(gain_own, sub)
        for l in range(sub):
            outf[pl.ds(base + spot * sub + l, share, stride=2 * sub), :] = out[:, l * lon_cols : (l + 1) * lon_cols]

    def settle(u):
        base = pl.multiple_of(lax.rem(u, 2) * lines, lines)
        out_blocks[u] = outf[pl.ds(base, lines), :].reshape(share, 2 * sub, lon_cols).astype(BF16)

    def pair(u, carry):
        settle(jnp.maximum(u - 1, 0))
        base = lax.rem(u, 2) * lines
        layers(2 * u + 1, hid_b, hid_a, 0, base)
        layers(jnp.minimum(2 * u + 2, tiles - 1), hid_a, hid_b, 1, base)
        return carry

    def embed(start, stop):
        lax.fori_loop(start, stop, pair, 0)

    hid_a[...] = half_silu(dot(w1p[...], xc[0]))
    outf[...] = jnp.zeros_like(outf)
    stops = FILL + (tiles // 2,)
    embed(0, stops[0])
    for copy in side_moves:
        copy.wait()
    corner_moves = [
        send(west.at[blocks - 1], corner.at[0], {"gx": down}),
        send(east.at[blocks - 1], corner.at[1], {"gx": down}),
        send(west.at[0], corner.at[2], {"gx": up}),
        send(east.at[0], corner.at[3], {"gx": up}),
    ]

    for copy in row_moves:
        copy.wait()
    half = KPAD * HALO
    xf[pl.ds(channels * HALO, (KPAD - channels) * HALO), :] = pad_values[0 : (KPAD - channels) * HALO] * 0.0 + jnp.where(
        lax.broadcasted_iota(jnp.int32, ((KPAD - channels) * HALO, 128), 0) < 3 * HALO, 1.0, 0.0
    ).astype(F32)
    for n, ref in enumerate((north, south)):
        xf[pl.ds(0, channels * HALO), :] = ref[...].astype(F32).reshape(channels * HALO, lon_cols)
        for l in range(HALO):
            xh[n, :, l * lon_cols : (l + 1) * lon_cols] = xf[pl.ds(l, KPAD, stride=HALO), :].astype(BF16)
    acc = gath[...]
    wing = HALO * lon_cols
    acc = acc + dot(xh[0], onehot(base_n, wing)) + dot(xh[1], onehot(base_s, wing))
    for ref, base in ((west, base_w), (east, base_e)):
        whole = jnp.concatenate([ref[i] for i in range(blocks)], axis=1)
        acc = acc + dot(whole, onehot(base, blocks * 128))
    gath[...] = acc
    embed(stops[0], stops[1])
    for copy in corner_moves:
        copy.wait()
    acc = gath[...]
    whole = jnp.concatenate([corner[i] for i in range(4)], axis=1)
    acc = acc + dot(whole, onehot(base_c, 4 * 128))
    picked = acc.astype(BF16)

    w2_in.wait()
    c, inv = centred(dot(w2_v[...], half_silu(dot(w1p[...], picked))))
    sender_latent = (c * inv * wide(cols[0], mine // 128)).astype(BF16)
    ew1_in.wait()
    for b in range(PARTS):
        pre_s[b] = dot(ew1_v[:, latent : 2 * latent], sender_latent[:, b * part : (b + 1) * part]) + wide(
            cols[1], part // 128
        )

    def edge_net(b):
        edge_in[b].wait()
        for copy in edge_moves[b]:
            copy.wait()
        pre = pre_s[b] + dot(ew1_v[:, :latent], edges[b])
        c, inv = centred(dot(ew2_v[...], half_silu(pre * 0.5)))
        part_sum = dot_nt((c * inv).astype(BF16), pick_s[b])
        tot[...] = part_sum if b == 0 else tot[...] + part_sum

    mesh_in.wait()
    for copy in mesh_moves:
        copy.wait()
    for b in range(PARTS):
        mesh_cols = dot(mesh_full[...], pick_s[b]).astype(BF16)
        pre_s[b] += dot(ew1_v[:, 2 * latent :], mesh_cols)
    ew2_in.wait()
    for b in range(PARTS):
        embed(stops[b + 1], stops[b + 2])
        edge_net(b)
    half = share // 2

    def sums(p, k):
        return tot[pl.ds(pl.multiple_of(p * share + k * half, 64), half), :]

    for k in range(2):
        tb[k] = sums(across, k).astype(BF16)
    tb[2] = sums(after, 1).astype(BF16)
    tb[3] = sums(before, 0).astype(BF16)
    relays = [send(tb.at[0], tr.at[0], {"gz": after}), send(tb.at[1], tr.at[1], {"gz": before})]
    sum_moves = [send(tb.at[2], tr.at[2], {"gz": after}), send(tb.at[3], tr.at[3], {"gz": before})]

    node_ids = lax.broadcasted_iota(jnp.int32, (nodes, slots), 0)
    slot_ids = lax.broadcasted_iota(jnp.int32, (nodes, slots), 1)
    pick = jnp.where((node_ids == recv_ref[...] - tile * nodes) & (slot_ids < live), 1.0, 0.0).astype(BF16)
    eown_in.wait()
    edge_sum = dot_nt(e_own[...], pick)
    degree = dot_nt(jnp.ones((8, slots), BF16), pick)[0:1, :]
    scale = 1.0 / jnp.maximum(degree, 1.0)
    gain_m = wide(cols[2, own(gz), :], nodes // 128)
    known = edge_sum + wide(cols[3, own(gz), :], nodes // 128) * degree
    mown_in.wait()
    spare = stops[PARTS + 1] + 1
    embed(stops[PARTS + 1], spare)
    for copy in relays:
        copy.wait()
    tb[4] = (sums(after, 0) + tr[0].astype(F32)).astype(BF16)
    tb[5] = (sums(before, 1) + tr[1].astype(F32)).astype(BF16)
    sum_moves += [send(tb.at[4], tr.at[4], {"gz": after}), send(tb.at[5], tr.at[5], {"gz": before})]
    embed(spare, stops[PARTS + 2])
    settle(tiles // 2 - 1)
    for copy in sum_moves:
        copy.wait()
    total = tot[own(gz), :] + jnp.concatenate(
        [tr[4].astype(F32) + tr[3].astype(F32), tr[2].astype(F32) + tr[5].astype(F32)], axis=0
    )
    out_mesh[...] = (mesh_own[...].astype(F32) + (known + gain_m * total) * scale).astype(BF16)


def deliver(mesh_ref, blocks_ref, out_mesh, out_grid, leave):
    count, _, rows, _ = blocks_ref.shape
    outs = [
        pltpu.make_async_copy(blocks_ref.at[u], out_grid.at[:, pl.ds(u * rows, rows), :], leave.at[u])
        for u in range(count)
    ]
    outs.append(pltpu.make_async_copy(mesh_ref, out_mesh, leave.at[count]))
    for copy in outs:
        copy.start()
    for copy in outs:
        copy.wait()


def on_device(
    sizes, grid_inputs, embed_w1, embed_b1, embed_w2, embed_gain, edge_w1, edge_b1, edge_w2,
    message_gain, message_bias, mesh_latent, edge_latent, senders, receivers, edge_counts,
):
    channels, lat_rows, lon_cols = grid_inputs.shape
    latent = embed_w2.shape[0]
    share, nodes, slots = mesh_latent.shape[0], mesh_latent.shape[3], edge_latent.shape[3]
    gz_n = sizes[2]
    mine = slots // gz_n
    blocks = lat_rows // ROWS
    tiles = lat_rows * lon_cols // TILE
    per = blocks and tiles // blocks
    anyspace = pl.BlockSpec(memory_space=pl.ANY)
    vmem = pl.BlockSpec(memory_space=pltpu.VMEM)
    smem = pl.BlockSpec(memory_space=pltpu.SMEM)
    V = pltpu.VMEM
    n_local = blocks + 1 + gz_n + 6 + PARTS + 7
    n_wire = PARTS * (gz_n - 1) + 20
    pairs, out_rows = tiles // 2, 2 * TILE // lon_cols
    mesh_out, grid_blocks = pl.pallas_call(
        functools.partial(kernel, sizes),
        out_shape=(
            pltpu.VMEM((share, nodes), BF16),
            pltpu.VMEM((pairs, share, out_rows, lon_cols), BF16),
        ),
        in_specs=[anyspace] * 14 + [smem],
        out_specs=(vmem, vmem),
        scratch_shapes=[
            V((blocks, channels, ROWS, lon_cols), BF16),
            V((channels, latent), BF16),
            V((latent, latent), BF16),
            V((latent, latent), BF16),
            V((latent, 3 * latent), BF16),
            V((latent, latent), BF16),
            V((share, slots), BF16),
            V((share, nodes), BF16),
            V((PARTS, latent, mine // PARTS), BF16),
            V((latent, nodes), BF16),
            V((channels, HALO, lon_cols), BF16),
            V((channels, HALO, lon_cols), BF16),
            V((blocks, KPAD, 128), BF16),
            V((blocks, KPAD, 128), BF16),
            V((4, KPAD, 128), BF16),
            V((KPAD * ROWS, lon_cols), F32),
            V((tiles, KPAD, TILE), BF16),
            V((2, KPAD, HALO * lon_cols), BF16),
            V((256, latent), F32),
            V((latent, KPAD), BF16),
            V((4, latent, 128), F32),
            V((per, TILE, 256), BF16),
            V((2, blocks, KPAD, 128), BF16),
            V((KPAD, mine), F32),
            V((2 * share * out_rows, lon_cols), F32),
            V((latent, nodes), F32),
            V((6, share // 2, nodes), BF16),
            V((6, share // 2, nodes), BF16),
            V((latent, TILE), BF16),
            V((latent, TILE), BF16),
            V((PARTS, latent, mine // PARTS), F32),
            V((PARTS, nodes, mine // PARTS), BF16),
            V((5, 1, latent), F32),
            V((1, slots), jnp.int32),
            V((1, slots), jnp.int32),
            pltpu.SemaphoreType.DMA((n_local,)),
            pltpu.SemaphoreType.DMA((n_wire,)),
            pltpu.SemaphoreType.DMA((n_wire,)),
        ],
        compiler_params=pltpu.CompilerParams(
            collective_id=0, has_side_effects=True, vmem_limit_bytes=56 * 1024 * 1024
        ),
    )(
        grid_inputs, embed_w1.T, embed_w2, edge_w1, edge_w2,
        embed_b1.reshape(1, latent), embed_gain.reshape(1, latent), edge_b1.reshape(1, latent),
        message_gain.reshape(1, latent), message_bias.reshape(1, latent),
        mesh_latent.reshape(share, nodes), edge_latent.reshape(share, slots),
        senders.reshape(1, slots), receivers.reshape(1, slots), edge_counts,
    )
    mesh_out, grid_out = pl.pallas_call(
        deliver,
        out_shape=(
            jax.ShapeDtypeStruct((share, nodes), BF16),
            jax.ShapeDtypeStruct((share, lat_rows, lon_cols), BF16),
        ),
        in_specs=[vmem, vmem],
        out_specs=(anyspace, anyspace),
        scratch_shapes=[pltpu.SemaphoreType.DMA((pairs + 1,))],
    )(
        pltpu.with_memory_space_constraint(mesh_out, pltpu.VMEM),
        pltpu.with_memory_space_constraint(grid_blocks, pltpu.VMEM),
    )
    return mesh_out.reshape(share, 1, 1, nodes), grid_out


def solution(mesh):
    sizes = (mesh.shape["gx"], mesh.shape["gy"], mesh.shape["gz"])
    return jax.shard_map(
        functools.partial(on_device, sizes),
        mesh=mesh,
        in_specs=(
            P(None, "gx", "gy"), P(), P(), P(), P(), P(), P(), P(), P(), P(),
            P("gz", "gx", "gy", None), P("gz", "gx", "gy", None),
            P("gx", "gy", None), P("gx", "gy", None), P("gx", "gy"),
        ),
        out_specs=(P("gz", "gx", "gy", None), P("gz", "gx", "gy")),
        check_vma=False,
    )
```
